32 devices in a mesh: groups: 2 (over y), seq: 4 (over x, core), tensor: 4 (over z).
Axes of the slice: x: 2, y: 2, z: 4, core: 2. Of those that a mesh axis runs over, the one named last changes fastest.
Arguments:
- hidden: bfloat16 [256, 4608], P(('groups', 'seq')), parts along dimension 0, may hold values from -6 to 6
- pre_gain: float32 [4608], replicated, may hold values from 0.25 to 1.75
- w_query: bfloat16 [4608, 4096], P(None, 'tensor'), may hold values from -0.09375 to 0.09375
- w_key: bfloat16 [4608, 2048], P(None, 'tensor'), may hold values from -0.09375 to 0.09375
- w_value: bfloat16 [4608, 2048], P(None, 'tensor'), may hold values from -0.09375 to 0.09375
- w_out: bfloat16 [4096, 4608], P('tensor'), may hold values from -0.125 to 0.125
- post_gain: float32 [4608], P('tensor'), may hold values from 0.25 to 1.75
- cache_pool: bfloat16 [512, 2, 128, 2048], P(('groups', 'seq'), None, None, 'tensor'), parts along dimension 0, may hold values from -6 to 6
- prompt_cache: bfloat16 [256, 2, 64, 2048], P('seq', None, None, 'tensor'), may hold values from -6 to 6
- task_ids: int32 [256], P('groups'), parts along dimension 0, may hold values from 0 to 255
- cache_lengths: int32 [256], P('groups'), parts along dimension 0, may hold values from 1 to 4096, as said below
- block_table: int32 [256, 32], P('groups'), parts along dimension 0, may hold values from -1 to 255, as said below
Outputs:
- layer_out: bfloat16 [256, 4608], P(('groups', 'seq'), 'tensor'), parts along dimension 0
- fresh_cache: bfloat16 [256, 2, 2048], P(('groups', 'seq'), None, 'tensor'), parts along dimension 0
The draws below stay inside these ranges and needn't reach their ends.
There are 2 independent parts, one for each index of `groups`. The reference program is written for one: setup_inputs(seed, part) draws one part's arguments, and reference() takes and returns one part's arrays. A program takes and returns all parts, laid end to end along the dimension named above; an argument that names none is the same for every part. Nothing has to cross between parts.
Inputs may be any that keep to these rules, and one draw needn't show every extreme that they name: `cache_lengths`: each draw has a request with exactly 4096 cache tokens. block_table[r, j] is the page of cache_pool holding cache tokens j * 128 to (j + 1) * 128 - 1 of request r for j < ceil(cache_lengths[r] / 128), and -1 for the later j; no page is named twice.
All inputs are finite; a program needn't handle non-finite values.
Results may differ from the reference program's by a relative error of at most 0.018.
Values may be sent and summed in bfloat16 or wider, within the bound.
No kernel may reach another device: no remote copies, remote signals or barrier semaphores. Data moves between devices by JAX's collectives and lax.ppermute only.
A program may use at most 128 MiB of HBM per device.

```python
import math
import jax
import jax.numpy as jnp
import numpy as np
from jax import lax

D = 4608
H = 32
KVH = 16
HD = 128
BLOCK = 128
PROMPT = 64
MAXLEN = 4096
MAXBLK = 32
TASKS = 256
REQ = 128
POOL = 256


def lengths_and_blocks(key):
    base = jax.random.fold_in(key, 7)
    k_first, k_second, k_order, k_tail, k_large, k_pages = jax.random.split(base, 6)
    extra = POOL - REQ - MAXBLK
    first_pick = jax.random.randint(k_first, (extra,), 0, REQ)
    second_pick = jax.random.randint(k_second, (extra,), 0, REQ)
    skewed = first_pick * second_pick // REQ
    order = jax.random.permutation(k_order, REQ)
    picked = order[skewed]
    counts = jnp.sum((picked[:, None] == jnp.arange(REQ)[None, :]).astype(jnp.int32), axis=0)
    largest = jax.random.randint(k_large, (), 0, REQ)
    is_large = jnp.arange(REQ) == largest
    blocks = jnp.where(is_large, MAXBLK, jnp.minimum(1 + counts, MAXBLK)).astype(jnp.int32)
    tails = jax.random.randint(k_tail, (REQ,), 1, BLOCK + 1)
    lengths = jnp.where(is_large, MAXLEN, (blocks - 1) * BLOCK + tails)
    offsets = jnp.cumsum(blocks) - blocks
    pages = jax.random.permutation(k_pages, POOL)
    slots = offsets[:, None] + jnp.arange(MAXBLK)[None, :]
    live_slot = jnp.arange(MAXBLK)[None, :] < blocks[:, None]
    table = jnp.where(live_slot, pages[jnp.minimum(slots, POOL - 1)], -1)
    return (lengths.astype(jnp.int32), table.astype(jnp.int32))


def draw_cache_lengths(key, part):
    return lengths_and_blocks(key)[0]


def draw_block_table(key, part):
    return lengths_and_blocks(key)[1]


def place_ends(values, own_key, least, high):
    longest = values.shape.index(max(values.shape))
    spots = []
    for shift in (0, 1):
        where = [jax.random.randint(jax.random.fold_in(own_key, axis), (), 0, length) for axis, length in enumerate(values.shape)]
        where[longest] = (where[longest] + shift) % values.shape[longest]
        spots.append(tuple(where))
    return values.at[spots[0]].set(least).at[spots[1]].set(high)


def spiked(drawn, stream_key, source, target, shards_of, factor):
    owner, partner = [(jnp.arange(drawn.shape[dim]) // (drawn.shape[dim] // shards_of)).reshape([-1 if axis == dim else 1 for axis in range(drawn.ndim)]) for dim in (source, target)]
    chosen = jax.random.permutation(stream_key, shards_of)[partner]
    strong = (owner == chosen) | (owner == (partner + shards_of // 2) % shards_of)
    return jnp.where(strong, factor * drawn, drawn)


def shard_levels(own_key, dims, pieces, low, high):
    loudness = 1.0
    for dim, shards_of in pieces:
        draws = jax.random.uniform(jax.random.fold_in(jax.random.fold_in(own_key, 6), dim), (shards_of,), jnp.float32, low / len(pieces), high / len(pieces))
        loudness = loudness * jnp.repeat(jnp.exp(draws), dims[dim] // shards_of).reshape((-1,) + (1,) * (len(dims) - 1 - dim))
    return loudness


def cumulative_ranks(amount, skew):
    portions = [(1 << 20) // math.isqrt(rank ** skew) + 1 for rank in range(1, amount + 1)]
    spread = 1 + sum(portions) // (1 << 30)
    return np.cumsum(np.array([max(1, weight // spread) for weight in portions]))


def skewed_ids(stream_key, dims, count, lean):
    grid = cumulative_ranks(count, lean)
    ticket = jax.random.randint(jax.random.fold_in(stream_key, 1), dims, 0, int(grid[count - 1]))
    grade = jnp.searchsorted(jnp.asarray(grid, jnp.int32), ticket, side="right")
    return jax.random.permutation(jax.random.fold_in(stream_key, 2), count)[grade].astype(jnp.int32)


def bell_draw(key, extent, scale, most, cuts=(), kind=jnp.bfloat16):
    level = shard_levels(key, extent, cuts, -0.22, 0.18) if cuts else 1.0
    values = jax.random.normal(key, extent, jnp.float32) * scale * level
    return jnp.minimum(jnp.maximum(values, -most), most).astype(kind)


def heavy_noise(stream_key, extent, spread, bound, pieces, heavy, kind=jnp.bfloat16):
    array = spread * jax.random.normal(stream_key, extent, jnp.float32)
    if pieces:
        array = array * shard_levels(stream_key, extent, pieces, -0.22, 0.18)
    return jnp.clip(spiked(array, jax.random.fold_in(stream_key, 3), *heavy), -bound, bound).astype(kind)


def setup_inputs(seed: int = 0, part: int = 0) -> dict:
    key_list = jax.random.split(jax.random.key(seed), 13)
    part_keys = jax.random.split(jax.random.fold_in(key_list[12], part), 13)
    hidden = bell_draw(part_keys[0], (REQ, D), 1.0, 6.0, ((0, 4),))
    pre_gain = jnp.clip(1.0 + 0.15 * jax.random.normal(key_list[1], (D,), jnp.float32), 0.25, 1.75)
    w_query = bell_draw(key_list[2], (D, H * HD), D ** -0.5, 0.09375, ((1, 4),))
    w_key = bell_draw(key_list[3], (D, KVH * HD), D ** -0.5, 0.09375, ((1, 4),))
    w_value = bell_draw(key_list[4], (D, KVH * HD), D ** -0.5, 0.09375, ((1, 4),))
    w_out = heavy_noise(key_list[5], (H * HD, D), (H * HD) ** -0.5, 0.125, ((0, 4),), (0, 1, 4, 2.0))
    post_gain = jnp.clip(1.0 + 0.15 * jax.random.normal(key_list[6], (D,), jnp.float32), 0.25, 1.75)
    cache_pool = bell_draw(part_keys[7], (POOL, 2, BLOCK, KVH * HD), 1.0, 6.0, ((0, 4), (3, 4)))
    prompt_cache = bell_draw(key_list[8], (TASKS, 2, PROMPT, KVH * HD), 1.0, 6.0, ((0, 4), (3, 4)))
    task_ids = place_ends(skewed_ids(part_keys[9], (REQ,), TASKS, 2), jax.random.fold_in(part_keys[9], 3), 0, TASKS - 1).astype(jnp.int32)
    cache_lengths = draw_cache_lengths(jax.random.fold_in(jax.random.fold_in(key_list[12], part), 71), part)
    block_table = draw_block_table(jax.random.fold_in(jax.random.fold_in(key_list[12], part), 71), part)
    return dict(hidden=hidden, pre_gain=pre_gain, w_query=w_query, w_key=w_key, w_value=w_value, w_out=w_out, post_gain=post_gain, cache_pool=cache_pool, prompt_cache=prompt_cache, task_ids=task_ids, cache_lengths=cache_lengths, block_table=block_table)


cap_limit = 50.0

def rms_scale(values, gain):
    mean_square = lax.optimization_barrier(jnp.mean(values * values, axis=-1, keepdims=True))
    return values * lax.rsqrt(mean_square + 1e-06) * gain

def rotate(values, position):
    half_dim = values.shape[-1] // 2
    frequency = 10000.0 ** (-jnp.arange(half_dim, dtype=jnp.float32) / half_dim)
    angles = position.astype(jnp.float32)[:, None] * frequency[None, :]
    cosine = jnp.cos(angles)[:, None, :]
    sines = jnp.sin(angles)[:, None, :]
    first_half = values[..., :half_dim]
    second_half = values[..., half_dim:]
    return jnp.concatenate([first_half * cosine - second_half * sines, second_half * cosine + first_half * sines], axis=-1)

def capped(raw_score, score_scale):
    return cap_limit * jnp.tanh(raw_score * score_scale / cap_limit)

def reference(hidden, pre_gain, w_query, w_key, w_value, w_out, post_gain, cache_pool, prompt_cache, task_ids, cache_lengths, block_table):
    normed = rms_scale(hidden.astype(jnp.float32), pre_gain.astype(jnp.float32)).astype(jnp.bfloat16)
    position = (PROMPT + cache_lengths).astype(jnp.int32)
    query_rows = rotate(jnp.dot(normed, w_query, preferred_element_type=jnp.float32).reshape(REQ, H, HD), position).astype(jnp.bfloat16)
    key_new = rotate(jnp.dot(normed, w_key, preferred_element_type=jnp.float32).reshape(REQ, KVH, HD), position).astype(jnp.bfloat16)
    value_new = jnp.dot(normed, w_value, preferred_element_type=jnp.float32).astype(jnp.bfloat16)
    fresh_cache = jnp.stack([key_new.reshape(REQ, KVH * HD), value_new], axis=1)
    score_scale = float(D // H) ** (-0.5)
    group_size = H // KVH

    def one_request(request_args):
        query_one, task_one, length_one, row_one, key_one, value_one = request_args
        request_pages = cache_pool[jnp.maximum(row_one, 0)]
        cache_keys = request_pages[:, 0].reshape(MAXBLK * BLOCK, KVH, HD)
        cache_values = request_pages[:, 1].reshape(MAXBLK * BLOCK, KVH, HD)
        prompt = prompt_cache[task_one]
        all_keys = jnp.concatenate([prompt[0].reshape(PROMPT, KVH, HD), cache_keys, key_one[None]], axis=0)
        all_values = jnp.concatenate([prompt[1].reshape(PROMPT, KVH, HD), cache_values, value_one.reshape(1, KVH, HD)], axis=0)
        key_mask = jnp.concatenate([jnp.ones((PROMPT,), bool), jnp.arange(MAXBLK * BLOCK) < length_one, jnp.ones((1,), bool)])
        grouped = query_one.reshape(KVH, group_size, HD).astype(jnp.float32)
        raw_score = jnp.einsum('kgd,tkd->kgt', grouped, all_keys.astype(jnp.float32))
        weight = jnp.where(key_mask[None, None, :], jnp.exp(capped(raw_score, score_scale)), 0.0)
        weight_sum = lax.optimization_barrier(jnp.sum(weight, axis=-1))
        rounded = lax.optimization_barrier(weight.astype(jnp.bfloat16)).astype(jnp.float32)
        mixture = jnp.einsum('kgt,tkd->kgd', rounded, all_values.astype(jnp.float32))
        return (mixture / weight_sum[..., None]).reshape(H * HD).astype(jnp.bfloat16)
    attended = lax.map(one_request, (query_rows, task_ids, cache_lengths, block_table, key_new, value_new))
    projected = jnp.dot(attended, w_out, preferred_element_type=jnp.float32)
    layer_out = hidden.astype(jnp.float32) + rms_scale(projected, post_gain.astype(jnp.float32))
    return (layer_out.astype(jnp.bfloat16), fresh_cache)
```

```python
import functools

import jax
import jax.numpy as jnp
from jax import lax
from jax.experimental import pallas as pl
from jax.experimental.pallas import tpu as pltpu
from jax.sharding import PartitionSpec as P

D = 4608
H = 32
HD = 128
LANES = 128
SUB = 8

cap_limit = 50.0
F32 = jnp.float32
BF16 = jnp.bfloat16


def rms_scale(values, gain):
    mean_square = jnp.mean(values * values, axis=-1, keepdims=True)
    return values * lax.rsqrt(mean_square + 1e-06) * gain


def rotate(values, position):
    half_dim = values.shape[-1] // 2
    frequency = 10000.0 ** (-jnp.arange(half_dim, dtype=jnp.float32) / half_dim)
    angles = position.astype(jnp.float32)[:, None] * frequency[None, :]
    cosine = jnp.cos(angles)[:, None, :]
    sines = jnp.sin(angles)[:, None, :]
    first_half = values[..., :half_dim]
    second_half = values[..., half_dim:]
    return jnp.concatenate(
        [first_half * cosine - second_half * sines, second_half * cosine + first_half * sines],
        axis=-1,
    )


def capped(raw_score, score_scale):
    return cap_limit * jnp.tanh(raw_score * score_scale / cap_limit)


def attend(query_block, block, live_mask, score_scale):
    count = block.shape[0]
    length = block.shape[2]
    kv_heads = query_block.shape[1]
    head_dim = query_block.shape[3]
    block_keys = block[:, 0].reshape(count, length, kv_heads, head_dim)
    block_values = block[:, 1].reshape(count, length, kv_heads, head_dim)
    raw_score = jnp.einsum(
        "nkgd,ntkd->nkgt", query_block, block_keys, preferred_element_type=jnp.float32
    )
    weight = jnp.where(live_mask[:, None, None, :], jnp.exp(capped(raw_score, score_scale)), 0.0)
    totals = jnp.sum(weight, axis=-1).reshape(count, -1)
    mixtures = jnp.einsum(
        "nkgt,ntkd->nkgd",
        weight.astype(jnp.bfloat16),
        block_values,
        preferred_element_type=jnp.float32,
    )
    return (totals, mixtures.reshape(count, -1))


def plain_body(
    hidden,
    pre_gain,
    w_query,
    w_key,
    w_value,
    w_out,
    post_gain,
    cache_pool,
    prompt_cache,
    task_ids,
    cache_lengths,
    block_table,
):
    seq_index = lax.axis_index("seq")
    tensor_index = lax.axis_index("tensor")
    own_rows = hidden.shape[0]
    requests = task_ids.shape[0]
    pages_dev = cache_pool.shape[0]
    block_len = cache_pool.shape[2]
    kv_width = cache_pool.shape[3]
    head_dim = HD
    kv_heads = kv_width // head_dim
    query_heads = w_query.shape[1] // head_dim
    group_size = query_heads // kv_heads
    prompt_len = prompt_cache.shape[2]
    tasks_dev = prompt_cache.shape[0]
    score_scale = float(D // H) ** (-0.5)
    first_row = seq_index * own_rows
    own_lengths = lax.dynamic_slice_in_dim(cache_lengths, first_row, own_rows)
    normed = rms_scale(hidden.astype(jnp.float32), pre_gain).astype(jnp.bfloat16)
    position = prompt_len + own_lengths
    query_rows = rotate(
        jnp.dot(normed, w_query, preferred_element_type=jnp.float32).reshape(
            own_rows, query_heads, head_dim
        ),
        position,
    ).astype(jnp.bfloat16)
    key_new = rotate(
        jnp.dot(normed, w_key, preferred_element_type=jnp.float32).reshape(
            own_rows, kv_heads, head_dim
        ),
        position,
    ).astype(jnp.bfloat16)
    value_new = jnp.dot(normed, w_value, preferred_element_type=jnp.float32).astype(jnp.bfloat16)
    fresh_cache = jnp.stack([key_new.reshape(own_rows, kv_width), value_new], axis=1)
    queries = lax.all_gather(
        query_rows.reshape(own_rows, query_heads * head_dim), "seq", axis=0, tiled=True
    )
    page_ids = seq_index * pages_dev + jnp.arange(pages_dev)
    flat_table = block_table.reshape(-1)
    max_blocks = block_table.shape[1]
    matches = flat_table[None, :] == page_ids[:, None]
    entry_index = jnp.arange(flat_table.shape[0])
    page_used = jnp.any(matches, axis=1)
    found_entry = jnp.sum(jnp.where(matches, entry_index[None, :], 0), axis=1)
    page_owner = found_entry // max_blocks
    block_number = found_entry % max_blocks
    owner_hot = (page_owner[:, None] == jnp.arange(requests)[None, :]) & page_used[:, None]
    owner_length = jnp.sum(jnp.where(owner_hot, cache_lengths[None, :], 0), axis=1)
    valid_count = jnp.clip(owner_length - block_number * block_len, 0, block_len)
    page_query = jnp.dot(
        owner_hot.astype(jnp.bfloat16), queries, preferred_element_type=jnp.float32
    ).astype(jnp.bfloat16)
    page_query = page_query.reshape(pages_dev, kv_heads, group_size, head_dim)
    page_live = jnp.arange(block_len)[None, :] < valid_count[:, None]
    page_totals, page_mixtures = attend(page_query, cache_pool, page_live, score_scale)
    spread_hot = owner_hot.astype(jnp.float32).T
    totals = jnp.dot(spread_hot, page_totals, precision=lax.Precision.HIGHEST)
    mixtures = jnp.dot(spread_hot, page_mixtures, precision=lax.Precision.HIGHEST)
    local_task = task_ids - seq_index * tasks_dev
    is_owned = (local_task >= 0) & (local_task < tasks_dev)
    task_rows = prompt_cache[jnp.clip(local_task, 0, tasks_dev - 1)]
    all_query = queries.reshape(requests, kv_heads, group_size, head_dim)
    owned_live = jnp.broadcast_to(is_owned[:, None], (requests, prompt_len))
    prompt_totals, prompt_mixtures = attend(all_query, task_rows, owned_live, score_scale)
    totals = totals + prompt_totals
    mixtures = mixtures + prompt_mixtures
    totals, mixtures = (
        lax.psum_scatter(
            totals.astype(jnp.bfloat16), "seq", scatter_dimension=0, tiled=True
        ).astype(jnp.float32),
        lax.psum_scatter(
            mixtures.astype(jnp.bfloat16), "seq", scatter_dimension=0, tiled=True
        ).astype(jnp.float32),
    )
    own_query = query_rows.reshape(own_rows, kv_heads, group_size, head_dim)
    self_raw = jnp.sum(
        own_query.astype(jnp.float32) * key_new[:, :, None, :].astype(jnp.float32), axis=-1
    )
    self_weight = jnp.exp(capped(self_raw, score_scale))
    rounded = lax.optimization_barrier(self_weight.astype(jnp.bfloat16)).astype(jnp.float32)
    totals = totals + self_weight.reshape(own_rows, -1)
    self_mix = rounded[..., None] * value_new.reshape(own_rows, kv_heads, 1, head_dim).astype(
        jnp.float32
    )
    mixtures = mixtures + self_mix.reshape(own_rows, -1)
    attended = (mixtures.reshape(own_rows, query_heads, head_dim) / totals[..., None]).astype(
        jnp.bfloat16
    )
    projected = jnp.dot(
        attended.reshape(own_rows, query_heads * head_dim),
        w_out,
        preferred_element_type=jnp.float32,
    )
    cols_local = post_gain.shape[0]
    col_start = tensor_index * cols_local
    residual = lax.dynamic_slice_in_dim(hidden, col_start, cols_local, 1).astype(jnp.float32)
    whole_sum = lax.psum(projected.astype(jnp.bfloat16), "tensor").astype(jnp.float32)
    mean_square = jnp.mean(whole_sum * whole_sum, axis=1, keepdims=True)
    scaled = lax.dynamic_slice_in_dim(whole_sum, col_start, cols_local, 1) * lax.rsqrt(
        mean_square + 1e-06
    )
    layer_out = (residual + scaled * post_gain).astype(jnp.bfloat16)
    return (layer_out, fresh_cache)


VM = pl.BlockSpec(memory_space=pltpu.VMEM)
SM = pl.BlockSpec(memory_space=pltpu.SMEM)
HB = pl.BlockSpec(memory_space=pltpu.HBM)


def cost(flops):
    return pl.CostEstimate(flops=flops, bytes_accessed=1 << 20, transcendentals=0)


def row_iota(rows):
    return lax.broadcasted_iota(jnp.int32, (rows, LANES), 0)


def lane_iota(rows):
    return lax.broadcasted_iota(jnp.int32, (rows, LANES), 1)


def query_kernel(prompt_len, chunks, lens_ref, hidden_ref, gain_ref, w_ref, q_ref, n_ref, cs_ref, w_buf, sem):
    rows, depth = hidden_ref.shape
    width = q_ref.shape[1]
    step = depth // chunks
    copies = []
    for c in range(chunks):
        part = pl.ds(c * step, step)
        copy = pltpu.make_async_copy(w_ref.at[part, :], w_buf.at[part, :], sem.at[c])
        copy.start()
        copies.append(copy)
    x = hidden_ref[...].astype(F32)
    mean_square = jnp.sum(x * x, axis=-1, keepdims=True) / depth
    n_ref[...] = (x * lax.rsqrt(mean_square + 1e-06) * gain_ref[...]).astype(BF16)
    first = lax.axis_index("seq") * rows
    row = row_iota(rows)
    lane = lane_iota(rows)
    length = jnp.zeros((rows, LANES), jnp.int32)
    for i in range(rows):
        length = jnp.where(row == i, lens_ref[first + i], length)
    half = LANES // 2
    low = lane < half
    slot = jnp.where(low, lane, lane - half).astype(F32)
    frequency = jnp.exp(slot * (-9.210340371976184 / half))
    angles = (length + prompt_len).astype(F32) * frequency
    cosine = jnp.cos(angles)
    sines = jnp.where(low, -jnp.sin(angles), jnp.sin(angles))
    cs_ref[:, :LANES] = cosine
    cs_ref[:, LANES:] = sines
    total = jnp.zeros((rows, width), F32)
    for c in range(chunks):
        copies[c].wait()
        total = total + jnp.dot(
            n_ref[:, c * step : (c + 1) * step],
            w_buf[c * step : (c + 1) * step, :],
            preferred_element_type=F32,
        )
    for h in range(width // LANES):
        v = total[:, h * LANES : (h + 1) * LANES]
        q_ref[:, h * LANES : (h + 1) * LANES] = (
            v * cosine + pltpu.roll(v, half, 1) * sines
        ).astype(BF16)


def plan_kernel(pages, block_len, tasks, table_ref, lens_ref, task_ref, meta_ref):
    requests = lens_ref.shape[0]
    seq = lax.axis_index("seq")
    page0 = seq * pages
    task0 = seq * tasks

    def clear(i, c):
        meta_ref[i] = 0
        return c

    lax.fori_loop(0, meta_ref.shape[0], clear, 0, unroll=8)

    def request(r, count):
        length = lens_ref[r]
        blocks = (length + block_len - 1) // block_len

        def block(j, c):
            page = table_ref[j, r] - page0

            @pl.when((page >= 0) & (page < pages))
            def _():
                meta_ref[page] = r
                meta_ref[pages + page] = jnp.minimum(length - j * block_len, block_len)

            return c

        lax.fori_loop(0, blocks, block, 0)
        task = task_ref[r] - task0
        here = (task >= 0) & (task < tasks)

        @pl.when(here)
        def _():
            meta_ref[2 * pages + count] = r
            meta_ref[2 * pages + requests + count] = task

        return count + here.astype(jnp.int32)

    count = lax.fori_loop(0, requests, request, 0)
    meta_ref[2 * pages + 2 * requests] = count


def attend_kernel(
    n_seq, score_scale, batch,
    meta_hbm, q_refs, pages_ref, prompt_ref, own_ref, msg_refs, meta_ref, qf, acc, acw, sem,
):
    rows, width = q_refs[0].shape
    heads = width // LANES
    pages, _, block_len, kv_width = pages_ref.shape
    kvh = kv_width // LANES
    group = heads // kvh
    prompt_len = prompt_ref.shape[2]
    requests = rows * n_seq
    me = lax.axis_index("seq")
    fetch = pltpu.make_async_copy(meta_hbm, meta_ref, sem)
    fetch.start()
    acc[...] = jnp.zeros_like(acc)
    acw[...] = jnp.zeros_like(acw)
    for k in range(n_seq):
        base = pl.multiple_of((me ^ k) * (rows * heads), SUB)
        for h in range(heads):
            qf[pl.ds(base + h, rows, stride=heads), :] = q_refs[k][
                :, h * LANES : (h + 1) * LANES
            ].astype(F32)
    fetch.wait()
    sub = row_iota(heads) // group
    lane = lane_iota(heads)
    zero = jnp.zeros((heads, LANES), F32)

    def spread(r):
        q = qf[pl.ds(pl.multiple_of(r * heads, SUB), heads), :]
        return jnp.concatenate([jnp.where(sub == g, q, zero) for g in range(kvh)], axis=1)

    def weigh(s, live):
        w = jnp.exp(cap_limit * jnp.tanh(s * (score_scale / cap_limit)))
        return jnp.where(live, w, zero)

    def collect(o):
        out = zero
        for g in range(kvh):
            out = jnp.where(sub == g, o[:, g * LANES : (g + 1) * LANES], out)
        return out

    def add(r, w, o):
        at = pl.ds(pl.multiple_of(r * heads, SUB), heads)
        acw[at, :] = acw[at, :] + w
        acc[at, :] = acc[at, :] + o

    pair = 2

    def page_step(i, c):
        owners, weights, values = [], [], []
        for b in range(batch):
            p = (i * batch + b) * pair
            who = [meta_ref[p + j] for j in range(pair)]
            q2 = jnp.concatenate([spread(r) for r in who], axis=0).astype(BF16)
            keys = pages_ref[pl.ds(p, pair), 0].reshape(pair * block_len, kv_width)
            s = lax.dot_general(q2, keys, (((1,), (1,)), ((), ())), preferred_element_type=F32)
            ws = []
            for j in range(pair):
                live = lane < meta_ref[pages + p + j]
                ws.append(weigh(s[j * heads : (j + 1) * heads, j * block_len : (j + 1) * block_len], live))
            owners.append(who)
            weights.append(ws)
        for b in range(batch):
            p = (i * batch + b) * pair
            ws = weights[b]
            w2 = jnp.concatenate(
                [
                    jnp.concatenate([ws[j] if m == j else zero for m in range(pair)], axis=1)
                    for j in range(pair)
                ],
                axis=0,
            ).astype(BF16)
            vals = pages_ref[pl.ds(p, pair), 1].reshape(pair * block_len, kv_width)
            values.append(jnp.dot(w2, vals, preferred_element_type=F32))
        for b in range(batch):
            for j in range(pair):
                add(owners[b][j], weights[b][j], collect(values[b][j * heads : (j + 1) * heads]))
        return c

    lax.fori_loop(0, pages // (pair * batch), page_step, 0)

    count = meta_ref[2 * pages + 2 * requests]
    per = LANES // prompt_len
    quad = 2 * per
    pbatch = 2

    def prompt_step(i, c):
        owners, weights, values, tasks = [], [], [], []
        for b in range(pbatch):
            e = (i * pbatch + b) * quad
            who = [meta_ref[2 * pages + e + j] for j in range(quad)]
            task = [meta_ref[2 * pages + requests + e + j] for j in range(quad)]
            q4 = jnp.concatenate([spread(r) for r in who], axis=0).astype(BF16)
            keys = jnp.concatenate([prompt_ref[t, 0] for t in task], axis=0)
            s = lax.dot_general(q4, keys, (((1,), (1,)), ((), ())), preferred_element_type=F32)
            ws = []
            for j in range(quad):
                tile = j // per
                live = (lane // prompt_len == j % per) & (e + j < count)
                ws.append(weigh(s[j * heads : (j + 1) * heads, tile * LANES : (tile + 1) * LANES], live))
            owners.append(who)
            weights.append(ws)
            tasks.append(task)
        for b in range(pbatch):
            ws = weights[b]
            w4 = jnp.concatenate(
                [
                    jnp.concatenate([ws[j] if m == j // per else zero for m in range(2)], axis=1)
                    for j in range(quad)
                ],
                axis=0,
            ).astype(BF16)
            vals = jnp.concatenate([prompt_ref[t, 1] for t in tasks[b]], axis=0)
            values.append(jnp.dot(w4, vals, preferred_element_type=F32))
        for b in range(pbatch):
            for j in range(quad):
                add(owners[b][j], weights[b][j], collect(values[b][j * heads : (j + 1) * heads]))
        return c

    lax.fori_loop(0, (count + quad * pbatch - 1) // (quad * pbatch), prompt_step, 0)

    lanes = lane_iota(rows)
    for k in range(n_seq):
        base = (me ^ k) * (rows * heads)
        sums = jnp.zeros((rows, LANES), F32)
        for h in range(heads):
            at = pl.ds(base + h, rows, stride=heads)
            mix = acc[at, :]
            tot = jnp.sum(acw[at, :], axis=1, keepdims=True)
            if k == 0:
                own_ref[:, h * LANES : (h + 1) * LANES] = mix
                sums = jnp.where(lanes == h, tot, sums)
            else:
                msg_refs[k - 1][:, h * LANES : (h + 1) * LANES] = mix.astype(BF16)
                top = tot.astype(BF16).astype(F32)
                sums = jnp.where(lanes == h, top, jnp.where(lanes == heads + h, tot - top, sums))
        if k == 0:
            own_ref[:, heads * LANES :] = sums
        else:
            msg_refs[k - 1][:, heads * LANES :] = sums.astype(BF16)


def fresh_kernel(score_scale, n_ref, cs_ref, q_ref, wk_ref, wv_ref, k_ref, v_ref, self_ref):
    rows, width = q_ref.shape
    heads = width // LANES
    kvh = k_ref.shape[1] // LANES
    group = heads // kvh
    half = LANES // 2
    normed = n_ref[...]
    cosine = cs_ref[:, :LANES]
    sines = cs_ref[:, LANES:]
    keys = jnp.dot(normed, wk_ref[...], preferred_element_type=F32)
    values = jnp.dot(normed, wv_ref[...], preferred_element_type=F32)
    lanes = lane_iota(rows)
    sums = jnp.zeros((rows, LANES), F32)
    for g in range(kvh):
        at = slice(g * LANES, (g + 1) * LANES)
        key = keys[:, at]
        key = (key * cosine + pltpu.roll(key, half, 1) * sines).astype(BF16)
        k_ref[:, at] = key
        key = key.astype(F32)
        val = values[:, at].astype(BF16)
        v_ref[:, at] = val
        val = val.astype(F32)
        for j in range(group):
            h = g * group + j
            raw = jnp.sum(q_ref[:, h * LANES : (h + 1) * LANES].astype(F32) * key, axis=1, keepdims=True)
            w = jnp.exp(cap_limit * jnp.tanh(raw * (score_scale / cap_limit)))
            self_ref[:, h * LANES : (h + 1) * LANES] = w.astype(BF16).astype(F32) * val
            sums = jnp.where(lanes == h, w, sums)
    self_ref[:, heads * LANES :] = sums


def project_kernel(n_ten, w_ref, own_ref, self_ref, got_refs, p0_ref, out_refs):
    rows, wide = own_ref.shape
    heads = wide // LANES - 1
    cols = p0_ref.shape[1]
    at = slice(heads * LANES, (heads + 1) * LANES)
    sums = own_ref[:, at] + self_ref[:, at]
    tail = None
    for r in got_refs:
        got = r[:, at].astype(F32)
        tail = got if tail is None else tail + got
    parts = []
    for h in range(heads):
        at = slice(h * LANES, (h + 1) * LANES)
        mix = own_ref[:, at] + self_ref[:, at]
        for r in got_refs:
            mix = mix + r[:, at].astype(F32)
        tot = sums[:, h : h + 1]
        if tail is not None:
            tot = tot + tail[:, h : h + 1] + tail[:, heads + h : heads + h + 1]
        parts.append((mix / tot).astype(BF16))
    att = jnp.concatenate(parts, axis=1)
    me = lax.axis_index("tensor")
    for k in range(n_ten):
        start = pl.multiple_of((me ^ k) * cols, LANES)
        got = jnp.dot(att, w_ref[:, pl.ds(start, cols)], preferred_element_type=F32)
        if k == 0:
            p0_ref[...] = got
        else:
            out_refs[k - 1][...] = got.astype(BF16)


def sum_kernel(p0_ref, got_refs, sum_ref, sq_ref):
    rows, cols = p0_ref.shape
    sq = jnp.zeros((rows, LANES), F32)
    for c in range(cols // LANES):
        at = slice(c * LANES, (c + 1) * LANES)
        t = p0_ref[:, at]
        for r in got_refs:
            t = t + r[:, at].astype(F32)
        sum_ref[:, at] = t
        sq = sq + t * t
    sq_ref[...] = sq


def last_kernel(sum_ref, sq_ref, got_refs, hidden_ref, gain_ref, out_ref):
    cols = out_ref.shape[1]
    sq = sq_ref[...]
    for r in got_refs:
        sq = sq + r[...]
    mean_square = jnp.sum(sq, axis=1, keepdims=True) / hidden_ref.shape[1]
    start = pl.multiple_of(lax.axis_index("tensor") * cols, LANES)
    residual = hidden_ref[:, pl.ds(start, cols)].astype(F32)
    out_ref[...] = (
        residual + sum_ref[...] * lax.rsqrt(mean_square + 1e-06) * gain_ref[...]
    ).astype(BF16)


def params(mib):
    return pltpu.CompilerParams(vmem_limit_bytes=mib << 20)


def swap(arrays, axis, size):
    return [
        lax.ppermute(a, axis, [(i, i ^ (k + 1)) for i in range(size)])
        for k, a in enumerate(arrays)
    ]


def shape(dims, dtype):
    return jax.ShapeDtypeStruct(dims, dtype)


def fast_body(
    n_seq,
    n_ten,
    hidden,
    pre_gain,
    w_query,
    w_key,
    w_value,
    w_out,
    post_gain,
    cache_pool,
    prompt_cache,
    task_ids,
    cache_lengths,
    block_table,
):
    rows, depth = hidden.shape
    width = w_query.shape[1]
    kv_width = w_key.shape[1]
    heads = width // LANES
    pages, _, block_len, _ = cache_pool.shape
    tasks, _, prompt_len, _ = prompt_cache.shape
    requests = task_ids.shape[0]
    cols = post_gain.shape[0]
    wide = width + LANES
    score_scale = float(D // H) ** (-0.5)
    chunks = 9 if depth % 9 == 0 else 1
    query, normed, cs = pl.pallas_call(
        functools.partial(query_kernel, prompt_len, chunks),
        out_shape=(shape((rows, width), BF16), shape((rows, depth), BF16), shape((rows, 2 * LANES), F32)),
        in_specs=[SM, VM, VM, HB],
        out_specs=(VM, VM, VM),
        scratch_shapes=[pltpu.VMEM((depth, width), BF16), pltpu.SemaphoreType.DMA((chunks,))],
        compiler_params=params(16),
        cost_estimate=cost(1 << 28),
        name="query",
    )(cache_lengths, hidden, pre_gain.reshape(1, depth), pltpu.with_memory_space_constraint(w_query, pltpu.HBM))
    got = swap([query] * (n_seq - 1), "seq", n_seq)
    meta_len = 2 * pages + 2 * requests + LANES
    meta = pl.pallas_call(
        functools.partial(plan_kernel, pages, block_len, tasks),
        out_shape=shape((meta_len,), jnp.int32),
        in_specs=[SM, SM, SM],
        out_specs=SM,
        compiler_params=params(1),
        cost_estimate=cost(1 << 28),
        name="plan",
    )(block_table.T, cache_lengths, task_ids)
    batch = 4
    outs = pl.pallas_call(
        lambda meta_r, q0, q1, q2, q3, pg, pr, own, m1, m2, m3, *scratch: attend_kernel(
            n_seq, score_scale, batch, meta_r, (q0, q1, q2, q3), pg, pr, own, (m1, m2, m3), *scratch
        ),
        out_shape=(shape((rows, wide), F32),) + (shape((rows, wide), BF16),) * (n_seq - 1),
        in_specs=[HB] + [VM] * (n_seq + 2),
        out_specs=(VM,) * n_seq,
        scratch_shapes=[
            pltpu.SMEM((meta_len,), jnp.int32),
            pltpu.VMEM((requests * heads, LANES), F32),
            pltpu.VMEM((requests * heads, LANES), F32),
            pltpu.VMEM((requests * heads, LANES), F32),
            pltpu.SemaphoreType.DMA,
        ],
        compiler_params=params(A_MIB),
        cost_estimate=cost(1 << 30),
        name="attend",
    )(meta, query, *got, cache_pool, prompt_cache)
    own, msgs = outs[0], outs[1:]
    got = swap(msgs, "seq", n_seq)
    key_new, value_new, self_part = pl.pallas_call(
        functools.partial(fresh_kernel, score_scale),
        out_shape=(shape((rows, kv_width), BF16), shape((rows, kv_width), BF16), shape((rows, wide), F32)),
        in_specs=[VM] * 5,
        out_specs=(VM,) * 3,
        compiler_params=params(G_MIB),
        cost_estimate=cost(1 << 29),
        name="fresh",
    )(normed, cs, query, w_key, w_value)
    outs = pl.pallas_call(
        lambda w, own, sf, r1, r2, r3, p0, o1, o2, o3: project_kernel(
            n_ten, w, own, sf, (r1, r2, r3), p0, (o1, o2, o3)
        ),
        out_shape=(shape((rows, cols), F32),) + (shape((rows, cols), BF16),) * (n_ten - 1),
        in_specs=[VM] * (3 + n_seq - 1),
        out_specs=(VM,) * n_ten,
        compiler_params=params(H_MIB),
        cost_estimate=cost(1 << 29),
        name="project",
    )(w_out, own, self_part, *got)
    p0, parts = outs[0], outs[1:]
    got = swap(parts, "tensor", n_ten)
    total, sq = pl.pallas_call(
        lambda p0, r1, r2, r3, t, s: sum_kernel(p0, (r1, r2, r3), t, s),
        out_shape=(shape((rows, cols), F32), shape((rows, LANES), F32)),
        in_specs=[VM] * n_ten,
        out_specs=(VM,) * 2,
        compiler_params=params(2),
        name="sum",
    )(p0, *got)
    got = swap([sq] * (n_ten - 1), "tensor", n_ten)
    layer_out = pl.pallas_call(
        lambda t, s, r1, r2, r3, hd, g, o: last_kernel(t, s, (r1, r2, r3), hd, g, o),
        out_shape=shape((rows, cols), BF16),
        in_specs=[VM] * (n_ten + 3),
        out_specs=VM,
        compiler_params=params(2),
        name="last",
    )(total, sq, *got, hidden, post_gain.reshape(1, cols))
    fresh_cache = jnp.stack([key_new, value_new], axis=1)
    return (layer_out, fresh_cache)


A_MIB = 6
G_MIB = 4
H_MIB = 4


def body(n_seq, n_ten, *args):
    hidden, w_query, post_gain, cache_pool, prompt_cache = args[0], args[2], args[6], args[7], args[8]
    fits = (
        n_seq == 4
        and n_ten == 4
        and w_query.shape[1] == SUB * HD
        and post_gain.shape[0] % LANES == 0
        and cache_pool.shape[2] == LANES
        and cache_pool.shape[0] % SUB == 0
        and LANES % prompt_cache.shape[2] == 0
        and prompt_cache.shape[2] % (2 * SUB) == 0
        and args[9].shape[0] == hidden.shape[0] * n_seq
        and hidden.shape[0] % (2 * SUB) == 0
    )
    if fits:
        return fast_body(n_seq, n_ten, *args)
    return plain_body(*args)


def solution(mesh):
    return jax.shard_map(
        functools.partial(body, mesh.shape["seq"], mesh.shape["tensor"]),
        mesh=mesh,
        in_specs=(
            P(("groups", "seq"), None),
            P(),
            P(None, "tensor"),
            P(None, "tensor"),
            P(None, "tensor"),
            P("tensor", None),
            P("tensor"),
            P(("groups", "seq"), None, None, "tensor"),
            P("seq", None, None, "tensor"),
            P("groups"),
            P("groups"),
            P("groups", None),
        ),
        out_specs=(P(("groups", "seq"), "tensor"), P(("groups", "seq"), None, "tensor")),
        check_vma=False,
    )
```

```python
import functools

import jax
import jax.numpy as jnp
from jax import lax
from jax.experimental import pallas as pl
from jax.experimental.pallas import tpu as pltpu
from jax.sharding import PartitionSpec as P

D = 4608
H = 32
HD = 128
LANES = 128
SUB = 8

cap_limit = 50.0
FLOPS_US = 1 << 30
BYTES_US = 1 << 20
F32 = jnp.float32
BF16 = jnp.bfloat16


def rms_scale(values, gain):
    mean_square = jnp.mean(values * values, axis=-1, keepdims=True)
    return values * lax.rsqrt(mean_square + 1e-06) * gain


def rotate(values, position):
    half_dim = values.shape[-1] // 2
    frequency = 10000.0 ** (-jnp.arange(half_dim, dtype=jnp.float32) / half_dim)
    angles = position.astype(jnp.float32)[:, None] * frequency[None, :]
    cosine = jnp.cos(angles)[:, None, :]
    sines = jnp.sin(angles)[:, None, :]
    first_half = values[..., :half_dim]
    second_half = values[..., half_dim:]
    return jnp.concatenate(
        [first_half * cosine - second_half * sines, second_half * cosine + first_half * sines],
        axis=-1,
    )


def capped(raw_score, score_scale):
    return cap_limit * jnp.tanh(raw_score * score_scale / cap_limit)


def attend(query_block, block, live_mask, score_scale):
    count = block.shape[0]
    length = block.shape[2]
    kv_heads = query_block.shape[1]
    head_dim = query_block.shape[3]
    block_keys = block[:, 0].reshape(count, length, kv_heads, head_dim)
    block_values = block[:, 1].reshape(count, length, kv_heads, head_dim)
    raw_score = jnp.einsum(
        "nkgd,ntkd->nkgt", query_block, block_keys, preferred_element_type=jnp.float32
    )
    weight = jnp.where(live_mask[:, None, None, :], jnp.exp(capped(raw_score, score_scale)), 0.0)
    totals = jnp.sum(weight, axis=-1).reshape(count, -1)
    mixtures = jnp.einsum(
        "nkgt,ntkd->nkgd",
        weight.astype(jnp.bfloat16),
        block_values,
        preferred_element_type=jnp.float32,
    )
    return (totals, mixtures.reshape(count, -1))


def plain_body(
    hidden,
    pre_gain,
    w_query,
    w_key,
    w_value,
    w_out,
    post_gain,
    cache_pool,
    prompt_cache,
    task_ids,
    cache_lengths,
    block_table,
):
    seq_index = lax.axis_index("seq")
    tensor_index = lax.axis_index("tensor")
    own_rows = hidden.shape[0]
    requests = task_ids.shape[0]
    pages_dev = cache_pool.shape[0]
    block_len = cache_pool.shape[2]
    kv_width = cache_pool.shape[3]
    head_dim = HD
    kv_heads = kv_width // head_dim
    query_heads = w_query.shape[1] // head_dim
    group_size = query_heads // kv_heads
    prompt_len = prompt_cache.shape[2]
    tasks_dev = prompt_cache.shape[0]
    score_scale = float(D // H) ** (-0.5)
    first_row = seq_index * own_rows
    own_lengths = lax.dynamic_slice_in_dim(cache_lengths, first_row, own_rows)
    normed = rms_scale(hidden.astype(jnp.float32), pre_gain).astype(jnp.bfloat16)
    position = prompt_len + own_lengths
    query_rows = rotate(
        jnp.dot(normed, w_query, preferred_element_type=jnp.float32).reshape(
            own_rows, query_heads, head_dim
        ),
        position,
    ).astype(jnp.bfloat16)
    key_new = rotate(
        jnp.dot(normed, w_key, preferred_element_type=jnp.float32).reshape(
            own_rows, kv_heads, head_dim
        ),
        position,
    ).astype(jnp.bfloat16)
    value_new = jnp.dot(normed, w_value, preferred_element_type=jnp.float32).astype(jnp.bfloat16)
    fresh_cache = jnp.stack([key_new.reshape(own_rows, kv_width), value_new], axis=1)
    queries = lax.all_gather(
        query_rows.reshape(own_rows, query_heads * head_dim), "seq", axis=0, tiled=True
    )
    page_ids = seq_index * pages_dev + jnp.arange(pages_dev)
    flat_table = block_table.reshape(-1)
    max_blocks = block_table.shape[1]
    matches = flat_table[None, :] == page_ids[:, None]
    entry_index = jnp.arange(flat_table.shape[0])
    page_used = jnp.any(matches, axis=1)
    found_entry = jnp.sum(jnp.where(matches, entry_index[None, :], 0), axis=1)
    page_owner = found_entry // max_blocks
    block_number = found_entry % max_blocks
    owner_hot = (page_owner[:, None] == jnp.arange(requests)[None, :]) & page_used[:, None]
    owner_length = jnp.sum(jnp.where(owner_hot, cache_lengths[None, :], 0), axis=1)
    valid_count = jnp.clip(owner_length - block_number * block_len, 0, block_len)
    page_query = jnp.dot(
        owner_hot.astype(jnp.bfloat16), queries, preferred_element_type=jnp.float32
    ).astype(jnp.bfloat16)
    page_query = page_query.reshape(pages_dev, kv_heads, group_size, head_dim)
    page_live = jnp.arange(block_len)[None, :] < valid_count[:, None]
    page_totals, page_mixtures = attend(page_query, cache_pool, page_live, score_scale)
    spread_hot = owner_hot.astype(jnp.float32).T
    totals = jnp.dot(spread_hot, page_totals, precision=lax.Precision.HIGHEST)
    mixtures = jnp.dot(spread_hot, page_mixtures, precision=lax.Precision.HIGHEST)
    local_task = task_ids - seq_index * tasks_dev
    is_owned = (local_task >= 0) & (local_task < tasks_dev)
    task_rows = prompt_cache[jnp.clip(local_task, 0, tasks_dev - 1)]
    all_query = queries.reshape(requests, kv_heads, group_size, head_dim)
    owned_live = jnp.broadcast_to(is_owned[:, None], (requests, prompt_len))
    prompt_totals, prompt_mixtures = attend(all_query, task_rows, owned_live, score_scale)
    totals = totals + prompt_totals
    mixtures = mixtures + prompt_mixtures
    totals, mixtures = (
        lax.psum_scatter(
            totals.astype(jnp.bfloat16), "seq", scatter_dimension=0, tiled=True
        ).astype(jnp.float32),
        lax.psum_scatter(
            mixtures.astype(jnp.bfloat16), "seq", scatter_dimension=0, tiled=True
        ).astype(jnp.float32),
    )
    own_query = query_rows.reshape(own_rows, kv_heads, group_size, head_dim)
    self_raw = jnp.sum(
        own_query.astype(jnp.float32) * key_new[:, :, None, :].astype(jnp.float32), axis=-1
    )
    self_weight = jnp.exp(capped(self_raw, score_scale))
    rounded = lax.optimization_barrier(self_weight.astype(jnp.bfloat16)).astype(jnp.float32)
    totals = totals + self_weight.reshape(own_rows, -1)
    self_mix = rounded[..., None] * value_new.reshape(own_rows, kv_heads, 1, head_dim).astype(
        jnp.float32
    )
    mixtures = mixtures + self_mix.reshape(own_rows, -1)
    attended = (mixtures.reshape(own_rows, query_heads, head_dim) / totals[..., None]).astype(
        jnp.bfloat16
    )
    projected = jnp.dot(
        attended.reshape(own_rows, query_heads * head_dim),
        w_out,
        preferred_element_type=jnp.float32,
    )
    cols_local = post_gain.shape[0]
    col_start = tensor_index * cols_local
    residual = lax.dynamic_slice_in_dim(hidden, col_start, cols_local, 1).astype(jnp.float32)
    whole_sum = lax.psum(projected.astype(jnp.bfloat16), "tensor").astype(jnp.float32)
    mean_square = jnp.mean(whole_sum * whole_sum, axis=1, keepdims=True)
    scaled = lax.dynamic_slice_in_dim(whole_sum, col_start, cols_local, 1) * lax.rsqrt(
        mean_square + 1e-06
    )
    layer_out = (residual + scaled * post_gain).astype(jnp.bfloat16)
    return (layer_out, fresh_cache)


VM = pl.BlockSpec(memory_space=pltpu.VMEM)
SM = pl.BlockSpec(memory_space=pltpu.SMEM)
HB = pl.BlockSpec(memory_space=pltpu.HBM)


def cost(us):
    return pl.CostEstimate(
        flops=int(us * FLOPS_US), bytes_accessed=int(us * BYTES_US), transcendentals=0
    )


def row_iota(rows):
    return lax.broadcasted_iota(jnp.int32, (rows, LANES), 0)


def lane_iota(rows):
    return lax.broadcasted_iota(jnp.int32, (rows, LANES), 1)


def query_kernel(
    prompt_len, chunks, lens_hbm, hidden_hbm, gain_hbm, w_ref, q_ref, n_ref, cs_ref,
    lens_ref, hidden_ref, gain_ref, w_buf, sem, small,
):
    rows, depth = hidden_ref.shape
    width = q_ref.shape[1]
    edges = [0]
    for c in chunks:
        edges.append(edges[-1] + c)
    first_copies = [
        pltpu.make_async_copy(hidden_hbm, hidden_ref, small.at[0]),
        pltpu.make_async_copy(gain_hbm, gain_ref, small.at[1]),
        pltpu.make_async_copy(lens_hbm, lens_ref, small.at[2]),
    ]
    for copy in first_copies:
        copy.start()
    copies = []
    for c in range(len(chunks)):
        part = pl.ds(edges[c], chunks[c])
        copies.append(pltpu.make_async_copy(w_ref.at[part, :], w_buf.at[part, :], sem.at[c]))
    for copy in copies[:AHEAD]:
        copy.start()
    for copy in first_copies:
        copy.wait()
    x = hidden_ref[...].astype(F32)
    mean_square = jnp.sum(x * x, axis=-1, keepdims=True) / depth
    gain = gain_ref[...].reshape(1, depth)
    n_ref[...] = (x * lax.rsqrt(mean_square + 1e-06) * gain).astype(BF16)
    first = lax.axis_index("seq") * rows
    row = row_iota(rows)
    lane = lane_iota(rows)
    length = jnp.zeros((rows, LANES), jnp.int32)
    for i in range(rows):
        length = jnp.where(row == i, lens_ref[first + i], length)
    half = LANES // 2
    low = lane < half
    slot = jnp.where(low, lane, lane - half).astype(F32)
    frequency = jnp.exp(slot * (-9.210340371976184 / half))
    angles = (length + prompt_len).astype(F32) * frequency
    cosine = jnp.cos(angles)
    sines = jnp.sin(angles)
    sines = jnp.where(low, -sines, sines)
    cs_ref[:, :LANES] = cosine
    cs_ref[:, LANES:] = sines
    total = jnp.zeros((rows, width), F32)
    for c in range(len(chunks)):
        copies[c].wait()
        if c + AHEAD < len(chunks):
            copies[c + AHEAD].start()
        total = total + jnp.dot(
            n_ref[:, edges[c] : edges[c + 1]],
            w_buf[edges[c] : edges[c + 1], :],
            preferred_element_type=F32,
        )
    for h in range(width // LANES):
        v = total[:, h * LANES : (h + 1) * LANES]
        q_ref[:, h * LANES : (h + 1) * LANES] = (
            v * cosine + pltpu.roll(v, half, 1) * sines
        ).astype(BF16)


CODE = 256
AHEAD = 3


def plan_kernel(pages, block_len, tasks, table_ref, lens_ref, task_ref, meta_ref):
    blocks, requests = table_ref.shape
    seq = lax.axis_index("seq")
    table = table_ref[...] - seq * pages
    lens = lens_ref[...]
    shape = (blocks, requests)
    block = lax.broadcasted_iota(jnp.int32, shape, 0)
    owner = lax.broadcasted_iota(jnp.int32, shape, 1)
    live = jnp.minimum(lens - block * block_len, block_len)
    code = jnp.where(live > 0, owner * CODE + live, 0)
    columns = []
    for p in range(pages):
        hit = jnp.where(table == p, code, 0)
        fold = hit[:SUB]
        for j in range(1, blocks // SUB):
            fold = fold + hit[j * SUB : (j + 1) * SUB]
        columns.append(jnp.sum(fold.astype(F32), axis=0, keepdims=True))
    found = jnp.sum(jnp.concatenate(columns, axis=0), axis=1, keepdims=True)
    at = lane_iota(pages) == row_iota(pages)
    first = jnp.sum(jnp.where(at, found, 0.0), axis=0, keepdims=True)
    task = task_ref[...] - seq * tasks
    here = (task >= 0) & (task < tasks)
    flag = jnp.broadcast_to(here.astype(F32), (SUB, requests))
    before = (
        lax.broadcasted_iota(jnp.int32, (requests, requests), 0)
        < lax.broadcasted_iota(jnp.int32, (requests, requests), 1)
    )
    rank = jnp.dot(flag.astype(BF16), before.astype(F32).astype(BF16), preferred_element_type=F32)[:1]
    item = lax.broadcasted_iota(jnp.int32, (requests, requests), 0)
    column = lax.broadcasted_iota(jnp.int32, (1, requests), 1)
    entry = (column * CODE + task).astype(F32)
    pick = (rank.astype(jnp.int32) == item) & here
    listed = jnp.sum(jnp.where(pick, entry, 0.0), axis=1, keepdims=True)
    same = item == lax.broadcasted_iota(jnp.int32, (requests, requests), 1)
    second = jnp.sum(jnp.where(same, listed, 0.0), axis=0, keepdims=True)
    count = jnp.sum(flag[:1], axis=1, keepdims=True)
    third = jnp.broadcast_to(count, (1, requests))
    rest = jnp.zeros((SUB - 3, requests), F32)
    meta_ref[...] = jnp.concatenate([first, second, third, rest], axis=0).astype(jnp.int32)


def attend_kernel(
    n_seq, score_scale, batch,
    meta_hbm, q_refs, pages_ref, prompt_ref, far_refs, own_ref, msg_refs, near_refs,
    meta_ref, qf, acc, acw, sem, far_sem,
):
    rows, width = q_refs[0].shape
    heads = width // LANES
    pages, _, block_len, kv_width = pages_ref.shape
    kvh = kv_width // LANES
    group = heads // kvh
    prompt_len = prompt_ref.shape[2]
    me = lax.axis_index("seq")
    fetch = pltpu.make_async_copy(meta_hbm, meta_ref, sem)
    fetch.start()
    loads = []
    for i, (far, near) in enumerate(zip(far_refs, near_refs)):
        loads.append(pltpu.make_async_copy(far, near, far_sem.at[i]))
        loads[-1].start()
    acc[...] = jnp.zeros_like(acc)
    acw[...] = jnp.zeros_like(acw)
    for k in range(n_seq):
        base = pl.multiple_of((me ^ k) * (rows * heads), SUB)
        for h in range(heads):
            qf[pl.ds(base + h, rows, stride=heads), :] = q_refs[k][
                :, h * LANES : (h + 1) * LANES
            ].astype(F32)
    fetch.wait()
    sub = row_iota(heads) // group
    lane = lane_iota(heads)
    zero = jnp.zeros((heads, LANES), F32)

    def spread(r):
        q = qf[pl.ds(pl.multiple_of(r * heads, SUB), heads), :]
        return jnp.concatenate([jnp.where(sub == g, q, zero) for g in range(kvh)], axis=1)

    def weigh(s, live):
        w = jnp.exp(cap_limit * jnp.tanh(s * (score_scale / cap_limit)))
        return jnp.where(live, w, zero)

    def collect(o):
        out = zero
        for g in range(kvh):
            out = jnp.where(sub == g, o[:, g * LANES : (g + 1) * LANES], out)
        return out

    def add(r, w, o):
        at = pl.ds(pl.multiple_of(r * heads, SUB), heads)
        acw[at, :] = acw[at, :] + w
        acc[at, :] = acc[at, :] + o

    pair = 2

    def page_step(i, c):
        owners, weights, values = [], [], []
        for b in range(batch):
            p = (i * batch + b) * pair
            note = [meta_ref[0, p + j] for j in range(pair)]
            who = [n // CODE for n in note]
            q2 = jnp.concatenate([spread(r) for r in who], axis=0).astype(BF16)
            keys = pages_ref[pl.ds(p, pair), 0].reshape(pair * block_len, kv_width)
            s = lax.dot_general(q2, keys, (((1,), (1,)), ((), ())), preferred_element_type=F32)
            ws = []
            for j in range(pair):
                live = lane < note[j] % CODE
                ws.append(weigh(s[j * heads : (j + 1) * heads, j * block_len : (j + 1) * block_len], live))
            owners.append(who)
            weights.append(ws)
        for b in range(batch):
            p = (i * batch + b) * pair
            ws = weights[b]
            w2 = jnp.concatenate(
                [
                    jnp.concatenate([ws[j] if m == j else zero for m in range(pair)], axis=1)
                    for j in range(pair)
                ],
                axis=0,
            ).astype(BF16)
            vals = pages_ref[pl.ds(p, pair), 1].reshape(pair * block_len, kv_width)
            values.append(jnp.dot(w2, vals, preferred_element_type=F32))
        for b in range(batch):
            for j in range(pair):
                add(owners[b][j], weights[b][j], collect(values[b][j * heads : (j + 1) * heads]))
        return c

    lax.fori_loop(0, pages // (pair * batch), page_step, 0)

    count = meta_ref[2, 0]
    per = LANES // prompt_len
    quad = 2 * per
    pbatch = 4

    def prompt_step(i, c):
        owners, weights, values, tasks = [], [], [], []
        for b in range(pbatch):
            e = (i * pbatch + b) * quad
            note = [meta_ref[1, e + j] for j in range(quad)]
            who = [n // CODE for n in note]
            task = [n % CODE for n in note]
            q4 = jnp.concatenate([spread(r) for r in who], axis=0).astype(BF16)
            keys = jnp.concatenate([prompt_ref[t, 0] for t in task], axis=0)
            s = lax.dot_general(q4, keys, (((1,), (1,)), ((), ())), preferred_element_type=F32)
            ws = []
            for j in range(quad):
                tile = j // per
                live = (lane // prompt_len == j % per) & (e + j < count)
                ws.append(weigh(s[j * heads : (j + 1) * heads, tile * LANES : (tile + 1) * LANES], live))
            owners.append(who)
            weights.append(ws)
            tasks.append(task)
        for b in range(pbatch):
            ws = weights[b]
            w4 = jnp.concatenate(
                [
                    jnp.concatenate([ws[j] if m == j // per else zero for m in range(2)], axis=1)
                    for j in range(quad)
                ],
                axis=0,
            ).astype(BF16)
            vals = jnp.concatenate([prompt_ref[t, 1] for t in tasks[b]], axis=0)
            values.append(jnp.dot(w4, vals, preferred_element_type=F32))
        for b in range(pbatch):
            for j in range(quad):
                add(owners[b][j], weights[b][j], collect(values[b][j * heads : (j + 1) * heads]))
        return c

    lax.fori_loop(0, (count + quad * pbatch - 1) // (quad * pbatch), prompt_step, 0)

    lanes = lane_iota(rows)
    for k in range(n_seq):
        base = (me ^ k) * (rows * heads)
        sums = jnp.zeros((rows, LANES), F32)
        for h in range(heads):
            at = pl.ds(base + h, rows, stride=heads)
            mix = acc[at, :]
            tot = jnp.sum(acw[at, :], axis=1, keepdims=True)
            if k == 0:
                own_ref[:, h * LANES : (h + 1) * LANES] = mix
                sums = jnp.where(lanes == h, tot, sums)
            else:
                msg_refs[k - 1][:, h * LANES : (h + 1) * LANES] = mix.astype(BF16)
                top = tot.astype(BF16).astype(F32)
                sums = jnp.where(lanes == h, top, jnp.where(lanes == heads + h, tot - top, sums))
        if k == 0:
            own_ref[:, heads * LANES :] = sums
        else:
            msg_refs[k - 1][:, heads * LANES :] = sums.astype(BF16)
    for load in loads:
        load.wait()


def fresh_kernel(
    score_scale, n_ref, cs_ref, q_ref, wk_ref, wv_hbm, k_ref, v_ref, self_ref, wv_ref, sem
):
    load = pltpu.make_async_copy(wv_hbm, wv_ref, sem)
    load.start()
    rows, width = q_ref.shape
    heads = width // LANES
    kvh = k_ref.shape[1] // LANES
    group = heads // kvh
    half = LANES // 2
    normed = n_ref[...]
    cosine = cs_ref[:, :LANES]
    sines = cs_ref[:, LANES:]
    keys = jnp.dot(normed, wk_ref[...], preferred_element_type=F32)
    load.wait()
    values = jnp.dot(normed, wv_ref[...], preferred_element_type=F32)
    lanes = lane_iota(rows)
    sums = jnp.zeros((rows, LANES), F32)
    for g in range(kvh):
        at = slice(g * LANES, (g + 1) * LANES)
        key = keys[:, at]
        key = (key * cosine + pltpu.roll(key, half, 1) * sines).astype(BF16)
        k_ref[:, at] = key
        key = key.astype(F32)
        val = values[:, at].astype(BF16)
        v_ref[:, at] = val
        val = val.astype(F32)
        for j in range(group):
            h = g * group + j
            raw = jnp.sum(q_ref[:, h * LANES : (h + 1) * LANES].astype(F32) * key, axis=1, keepdims=True)
            w = jnp.exp(cap_limit * jnp.tanh(raw * (score_scale / cap_limit)))
            self_ref[:, h * LANES : (h + 1) * LANES] = w.astype(BF16).astype(F32) * val
            sums = jnp.where(lanes == h, w, sums)
    self_ref[:, heads * LANES :] = sums


def project_kernel(n_ten, w_ref, own_ref, self_ref, got_refs, p0_ref, out_refs):
    _, wide = own_ref.shape
    heads = wide // LANES - 1
    cols = p0_ref.shape[1]
    at = slice(heads * LANES, (heads + 1) * LANES)
    sums = own_ref[:, at] + self_ref[:, at]
    tail = None
    for r in got_refs:
        got = r[:, at].astype(F32)
        tail = got if tail is None else tail + got
    parts = []
    for h in range(heads):
        at = slice(h * LANES, (h + 1) * LANES)
        mix = own_ref[:, at] + self_ref[:, at]
        for r in got_refs:
            mix = mix + r[:, at].astype(F32)
        tot = sums[:, h : h + 1]
        if tail is not None:
            tot = tot + tail[:, h : h + 1] + tail[:, heads + h : heads + h + 1]
        parts.append((mix / tot).astype(BF16))
    att = jnp.concatenate(parts, axis=1)
    me = lax.axis_index("tensor")
    for k in range(n_ten):
        start = pl.multiple_of((me ^ k) * cols, LANES)
        got = jnp.dot(att, w_ref[:, pl.ds(start, cols)], preferred_element_type=F32)
        if k == 0:
            p0_ref[...] = got
        else:
            out_refs[k - 1][...] = got.astype(BF16)


def sum_kernel(p0_ref, got_refs, sum_ref, sq_ref):
    rows, cols = p0_ref.shape
    sq = jnp.zeros((rows, LANES), F32)
    for c in range(cols // LANES):
        at = slice(c * LANES, (c + 1) * LANES)
        t = p0_ref[:, at]
        for r in got_refs:
            t = t + r[:, at].astype(F32)
        sum_ref[:, at] = t
        sq = sq + t * t
    sq_ref[...] = sq


def last_kernel(sum_ref, sq_ref, got_refs, hidden_ref, gain_ref, out_ref):
    cols = out_ref.shape[1]
    sq = sq_ref[...]
    for r in got_refs:
        sq = sq + r[...]
    mean_square = jnp.sum(sq, axis=1, keepdims=True) / hidden_ref.shape[1]
    start = pl.multiple_of(lax.axis_index("tensor") * cols, LANES)
    residual = hidden_ref[:, pl.ds(start, cols)].astype(F32)
    out_ref[...] = (
        residual + sum_ref[...] * lax.rsqrt(mean_square + 1e-06) * gain_ref[...]
    ).astype(BF16)


def params(mib):
    return pltpu.CompilerParams(vmem_limit_bytes=mib << 20)


def swap(arrays, axis, size):
    got = []
    for k, a in enumerate(arrays):
        got.append(lax.ppermute(a, axis, [(i, i ^ (k + 1)) for i in range(size)]))
    return got


def split(depth, count):
    unit = 2 * LANES
    step = max(1, depth // (unit * count)) * unit
    edges = list(range(0, depth - step + 1, step)) + [depth]
    return tuple(b - a for a, b in zip(edges, edges[1:]))


def in_hbm(array):
    return pltpu.with_memory_space_constraint(array, pltpu.HBM)


def shape(dims, dtype):
    return jax.ShapeDtypeStruct(dims, dtype)


def fast_body(
    n_seq,
    n_ten,
    hidden,
    pre_gain,
    w_query,
    w_key,
    w_value,
    w_out,
    post_gain,
    cache_pool,
    prompt_cache,
    task_ids,
    cache_lengths,
    block_table,
):
    rows, depth = hidden.shape
    width = w_query.shape[1]
    kv_width = w_key.shape[1]
    heads = width // LANES
    pages, _, block_len, _ = cache_pool.shape
    tasks, _, prompt_len, _ = prompt_cache.shape
    requests = task_ids.shape[0]
    cols = post_gain.shape[0]
    wide = width + LANES
    score_scale = float(D // H) ** (-0.5)
    chunks = split(depth, 6)
    query, normed, cs = pl.pallas_call(
        functools.partial(query_kernel, prompt_len, chunks),
        out_shape=(
            pltpu.VMEM((rows, width), BF16),
            pltpu.VMEM((rows, depth), BF16),
            pltpu.VMEM((rows, 2 * LANES), F32),
        ),
        in_specs=[HB] * 4,
        out_specs=(VM, VM, VM),
        scratch_shapes=[
            pltpu.SMEM((requests,), jnp.int32),
            pltpu.VMEM((rows, depth), BF16),
            pltpu.VMEM((depth,), F32),
            pltpu.VMEM((depth, width), BF16),
            pltpu.SemaphoreType.DMA((len(chunks),)),
            pltpu.SemaphoreType.DMA((3,)),
        ],
        compiler_params=params(Q_MIB),
        cost_estimate=cost(0.05),
        name="query",
    )(*[in_hbm(a) for a in (cache_lengths, hidden, pre_gain, w_query)])
    query = pl.pallas_call(
        lambda q, o: None,
        out_shape=pltpu.VMEM((rows, width), BF16),
        in_specs=[VM],
        out_specs=VM,
        input_output_aliases={0: 0},
        compiler_params=params(1),
        cost_estimate=cost(12),
        name="gate",
    )(query)
    got = swap([query] * (n_seq - 1), "seq", n_seq)
    meta = pl.pallas_call(
        functools.partial(plan_kernel, pages, block_len, tasks),
        out_shape=shape((SUB, requests), jnp.int32),
        in_specs=[VM, VM, VM],
        out_specs=VM,
        compiler_params=params(1),
        cost_estimate=cost(9),
        name="plan",
    )(block_table.T, cache_lengths.reshape(1, requests), task_ids.reshape(1, requests))
    batch = 32
    outs = pl.pallas_call(
        lambda meta_r, q0, q1, q2, q3, pg, pr, f1, f2, own, m1, m2, m3, n1, n2, *scratch: attend_kernel(
            n_seq, score_scale, batch, meta_r, (q0, q1, q2, q3), pg, pr, (f1, f2),
            own, (m1, m2, m3), (n1, n2), *scratch
        ),
        out_shape=(shape((rows, wide), F32),)
        + (shape((rows, wide), BF16),) * (n_seq - 1)
        + tuple(pltpu.VMEM(w.shape, w.dtype) for w in (w_key, w_out)),
        in_specs=[HB] + [VM] * (n_seq + 2) + [HB] * 2,
        out_specs=(VM,) * (n_seq + 2),
        scratch_shapes=[
            pltpu.SMEM((SUB, requests), jnp.int32),
            pltpu.VMEM((requests * heads, LANES), F32),
            pltpu.VMEM((requests * heads, LANES), F32),
            pltpu.VMEM((requests * heads, LANES), F32),
            pltpu.SemaphoreType.DMA,
            pltpu.SemaphoreType.DMA((2,)),
        ],
        compiler_params=params(A_MIB),
        cost_estimate=cost(8),
        name="attend",
    )(meta, query, *got, cache_pool, prompt_cache, in_hbm(w_key), in_hbm(w_out))
    own, msgs = outs[0], outs[1:n_seq]
    key_near, out_near = outs[n_seq:]
    got = swap(msgs, "seq", n_seq)
    key_new, value_new, self_part = pl.pallas_call(
        functools.partial(fresh_kernel, score_scale),
        out_shape=(shape((rows, kv_width), BF16), shape((rows, kv_width), BF16), shape((rows, wide), F32)),
        in_specs=[VM] * 4 + [HB],
        out_specs=(VM,) * 3,
        scratch_shapes=[pltpu.VMEM(w_value.shape, BF16), pltpu.SemaphoreType.DMA],
        compiler_params=params(G_MIB),
        cost_estimate=cost(1.7),
        name="fresh",
    )(normed, cs, query, key_near, in_hbm(w_value))
    outs = pl.pallas_call(
        lambda w, own, sf, r1, r2, r3, p0, o1, o2, o3: project_kernel(
            n_ten, w, own, sf, (r1, r2, r3), p0, (o1, o2, o3)
        ),
        out_shape=(shape((rows, cols), F32),) + (shape((rows, cols), BF16),) * (n_ten - 1),
        in_specs=[VM] * (3 + n_seq - 1),
        out_specs=(VM,) * n_ten,
        compiler_params=params(H_MIB),
        cost_estimate=cost(1.9),
        name="project",
    )(out_near, own, self_part, *got)
    p0, parts = outs[0], outs[1:]
    got = swap(parts, "tensor", n_ten)
    total, sq = pl.pallas_call(
        lambda p0, r1, r2, r3, t, s: sum_kernel(p0, (r1, r2, r3), t, s),
        out_shape=(shape((rows, cols), F32), shape((rows, LANES), F32)),
        in_specs=[VM] * n_ten,
        out_specs=(VM,) * 2,
        compiler_params=params(2),
        cost_estimate=cost(0.3),
        name="sum",
    )(p0, *got)
    got = swap([sq] * (n_ten - 1), "tensor", n_ten)
    layer_out = pl.pallas_call(
        lambda t, s, r1, r2, r3, hd, g, o: last_kernel(t, s, (r1, r2, r3), hd, g, o),
        out_shape=shape((rows, cols), BF16),
        in_specs=[VM] * (n_ten + 3),
        out_specs=VM,
        compiler_params=params(2),
        cost_estimate=cost(0.3),
        name="last",
    )(total, sq, *got, hidden, post_gain.reshape(1, cols))
    fresh_cache = jnp.stack([key_new, value_new], axis=1)
    return (layer_out, fresh_cache)


Q_MIB = 60
A_MIB = 6
G_MIB = 9
H_MIB = 4


def body(n_seq, n_ten, *args):
    hidden, w_query, post_gain, cache_pool, prompt_cache = args[0], args[2], args[6], args[7], args[8]
    fits = (
        n_seq == 4
        and n_ten == 4
        and w_query.shape[1] == SUB * HD
        and post_gain.shape[0] % LANES == 0
        and cache_pool.shape[2] == LANES
        and cache_pool.shape[0] % SUB == 0
        and LANES % prompt_cache.shape[2] == 0
        and prompt_cache.shape[2] % (2 * SUB) == 0
        and args[9].shape[0] == LANES == hidden.shape[0] * n_seq
        and args[11].shape[1] % SUB == 0
        and prompt_cache.shape[0] <= CODE
        and cache_pool.shape[0] <= LANES
        and hidden.shape[0] % (2 * SUB) == 0
    )
    if fits:
        return fast_body(n_seq, n_ten, *args)
    return plain_body(*args)


def solution(mesh):
    return jax.shard_map(
        functools.partial(body, mesh.shape["seq"], mesh.shape["tensor"]),
        mesh=mesh,
        in_specs=(
            P(("groups", "seq"), None),
            P(),
            P(None, "tensor"),
            P(None, "tensor"),
            P(None, "tensor"),
            P("tensor", None),
            P("tensor"),
            P(("groups", "seq"), None, None, "tensor"),
            P("seq", None, None, "tensor"),
            P("groups"),
            P("groups"),
            P("groups", None),
        ),
        out_specs=(P(("groups", "seq"), "tensor"), P(("groups", "seq"), None, "tensor")),
        check_vma=False,
    )
```

```python
import functools

import jax
import jax.numpy as jnp
from jax import lax
from jax.experimental import pallas as pl
from jax.experimental.pallas import tpu as pltpu
from jax.sharding import PartitionSpec as P

D = 4608
H = 32
HD = 128
LANES = 128
SUB = 8

cap_limit = 50.0
FLOPS_US = 1 << 30
BYTES_US = 1 << 20
F32 = jnp.float32
BF16 = jnp.bfloat16


def rms_scale(values, gain):
    mean_square = jnp.mean(values * values, axis=-1, keepdims=True)
    return values * lax.rsqrt(mean_square + 1e-06) * gain


def rotate(values, position):
    half_dim = values.shape[-1] // 2
    frequency = 10000.0 ** (-jnp.arange(half_dim, dtype=jnp.float32) / half_dim)
    angles = position.astype(jnp.float32)[:, None] * frequency[None, :]
    cosine = jnp.cos(angles)[:, None, :]
    sines = jnp.sin(angles)[:, None, :]
    first_half = values[..., :half_dim]
    second_half = values[..., half_dim:]
    return jnp.concatenate(
        [first_half * cosine - second_half * sines, second_half * cosine + first_half * sines],
        axis=-1,
    )


def capped(raw_score, score_scale):
    return cap_limit * jnp.tanh(raw_score * score_scale / cap_limit)


def attend(query_block, block, live_mask, score_scale):
    count = block.shape[0]
    length = block.shape[2]
    kv_heads = query_block.shape[1]
    head_dim = query_block.shape[3]
    block_keys = block[:, 0].reshape(count, length, kv_heads, head_dim)
    block_values = block[:, 1].reshape(count, length, kv_heads, head_dim)
    raw_score = jnp.einsum(
        "nkgd,ntkd->nkgt", query_block, block_keys, preferred_element_type=jnp.float32
    )
    weight = jnp.where(live_mask[:, None, None, :], jnp.exp(capped(raw_score, score_scale)), 0.0)
    totals = jnp.sum(weight, axis=-1).reshape(count, -1)
    mixtures = jnp.einsum(
        "nkgt,ntkd->nkgd",
        weight.astype(jnp.bfloat16),
        block_values,
        preferred_element_type=jnp.float32,
    )
    return (totals, mixtures.reshape(count, -1))


def plain_body(
    hidden,
    pre_gain,
    w_query,
    w_key,
    w_value,
    w_out,
    post_gain,
    cache_pool,
    prompt_cache,
    task_ids,
    cache_lengths,
    block_table,
):
    seq_index = lax.axis_index("seq")
    tensor_index = lax.axis_index("tensor")
    own_rows = hidden.shape[0]
    requests = task_ids.shape[0]
    pages_dev = cache_pool.shape[0]
    block_len = cache_pool.shape[2]
    kv_width = cache_pool.shape[3]
    head_dim = HD
    kv_heads = kv_width // head_dim
    query_heads = w_query.shape[1] // head_dim
    group_size = query_heads // kv_heads
    prompt_len = prompt_cache.shape[2]
    tasks_dev = prompt_cache.shape[0]
    score_scale = float(D // H) ** (-0.5)
    first_row = seq_index * own_rows
    own_lengths = lax.dynamic_slice_in_dim(cache_lengths, first_row, own_rows)
    normed = rms_scale(hidden.astype(jnp.float32), pre_gain).astype(jnp.bfloat16)
    position = prompt_len + own_lengths
    query_rows = rotate(
        jnp.dot(normed, w_query, preferred_element_type=jnp.float32).reshape(
            own_rows, query_heads, head_dim
        ),
        position,
    ).astype(jnp.bfloat16)
    key_new = rotate(
        jnp.dot(normed, w_key, preferred_element_type=jnp.float32).reshape(
            own_rows, kv_heads, head_dim
        ),
        position,
    ).astype(jnp.bfloat16)
    value_new = jnp.dot(normed, w_value, preferred_element_type=jnp.float32).astype(jnp.bfloat16)
    fresh_cache = jnp.stack([key_new.reshape(own_rows, kv_width), value_new], axis=1)
    queries = lax.all_gather(
        query_rows.reshape(own_rows, query_heads * head_dim), "seq", axis=0, tiled=True
    )
    page_ids = seq_index * pages_dev + jnp.arange(pages_dev)
    flat_table = block_table.reshape(-1)
    max_blocks = block_table.shape[1]
    matches = flat_table[None, :] == page_ids[:, None]
    entry_index = jnp.arange(flat_table.shape[0])
    page_used = jnp.any(matches, axis=1)
    found_entry = jnp.sum(jnp.where(matches, entry_index[None, :], 0), axis=1)
    page_owner = found_entry // max_blocks
    block_number = found_entry % max_blocks
    owner_hot = (page_owner[:, None] == jnp.arange(requests)[None, :]) & page_used[:, None]
    owner_length = jnp.sum(jnp.where(owner_hot, cache_lengths[None, :], 0), axis=1)
    valid_count = jnp.clip(owner_length - block_number * block_len, 0, block_len)
    page_query = jnp.dot(
        owner_hot.astype(jnp.bfloat16), queries, preferred_element_type=jnp.float32
    ).astype(jnp.bfloat16)
    page_query = page_query.reshape(pages_dev, kv_heads, group_size, head_dim)
    page_live = jnp.arange(block_len)[None, :] < valid_count[:, None]
    page_totals, page_mixtures = attend(page_query, cache_pool, page_live, score_scale)
    spread_hot = owner_hot.astype(jnp.float32).T
    totals = jnp.dot(spread_hot, page_totals, precision=lax.Precision.HIGHEST)
    mixtures = jnp.dot(spread_hot, page_mixtures, precision=lax.Precision.HIGHEST)
    local_task = task_ids - seq_index * tasks_dev
    is_owned = (local_task >= 0) & (local_task < tasks_dev)
    task_rows = prompt_cache[jnp.clip(local_task, 0, tasks_dev - 1)]
    all_query = queries.reshape(requests, kv_heads, group_size, head_dim)
    owned_live = jnp.broadcast_to(is_owned[:, None], (requests, prompt_len))
    prompt_totals, prompt_mixtures = attend(all_query, task_rows, owned_live, score_scale)
    totals = totals + prompt_totals
    mixtures = mixtures + prompt_mixtures
    totals, mixtures = (
        lax.psum_scatter(
            totals.astype(jnp.bfloat16), "seq", scatter_dimension=0, tiled=True
        ).astype(jnp.float32),
        lax.psum_scatter(
            mixtures.astype(jnp.bfloat16), "seq", scatter_dimension=0, tiled=True
        ).astype(jnp.float32),
    )
    own_query = query_rows.reshape(own_rows, kv_heads, group_size, head_dim)
    self_raw = jnp.sum(
        own_query.astype(jnp.float32) * key_new[:, :, None, :].astype(jnp.float32), axis=-1
    )
    self_weight = jnp.exp(capped(self_raw, score_scale))
    rounded = lax.optimization_barrier(self_weight.astype(jnp.bfloat16)).astype(jnp.float32)
    totals = totals + self_weight.reshape(own_rows, -1)
    self_mix = rounded[..., None] * value_new.reshape(own_rows, kv_heads, 1, head_dim).astype(
        jnp.float32
    )
    mixtures = mixtures + self_mix.reshape(own_rows, -1)
    attended = (mixtures.reshape(own_rows, query_heads, head_dim) / totals[..., None]).astype(
        jnp.bfloat16
    )
    projected = jnp.dot(
        attended.reshape(own_rows, query_heads * head_dim),
        w_out,
        preferred_element_type=jnp.float32,
    )
    cols_local = post_gain.shape[0]
    col_start = tensor_index * cols_local
    residual = lax.dynamic_slice_in_dim(hidden, col_start, cols_local, 1).astype(jnp.float32)
    whole_sum = lax.psum(projected.astype(jnp.bfloat16), "tensor").astype(jnp.float32)
    mean_square = jnp.mean(whole_sum * whole_sum, axis=1, keepdims=True)
    scaled = lax.dynamic_slice_in_dim(whole_sum, col_start, cols_local, 1) * lax.rsqrt(
        mean_square + 1e-06
    )
    layer_out = (residual + scaled * post_gain).astype(jnp.bfloat16)
    return (layer_out, fresh_cache)


VM = pl.BlockSpec(memory_space=pltpu.VMEM)
SM = pl.BlockSpec(memory_space=pltpu.SMEM)
HB = pl.BlockSpec(memory_space=pltpu.HBM)


def cost(us):
    return pl.CostEstimate(
        flops=int(us * FLOPS_US), bytes_accessed=int(us * BYTES_US), transcendentals=0
    )


def row_iota(rows):
    return lax.broadcasted_iota(jnp.int32, (rows, LANES), 0)


def lane_iota(rows):
    return lax.broadcasted_iota(jnp.int32, (rows, LANES), 1)


def query_kernel(
    prompt_len, chunks, lens_hbm, hidden_hbm, gain_hbm, w_ref, q_ref, n_ref, cs_ref,
    lens_ref, hidden_ref, gain_ref, w_buf, sem, small,
):
    rows, depth = hidden_ref.shape
    width = q_ref.shape[1]
    edges = [0]
    for c in chunks:
        edges.append(edges[-1] + c)
    first_copies = [
        pltpu.make_async_copy(hidden_hbm, hidden_ref, small.at[0]),
        pltpu.make_async_copy(gain_hbm, gain_ref, small.at[1]),
        pltpu.make_async_copy(lens_hbm, lens_ref, small.at[2]),
    ]
    for copy in first_copies:
        copy.start()
    copies = []
    for c in range(len(chunks)):
        part = pl.ds(edges[c], chunks[c])
        copies.append(pltpu.make_async_copy(w_ref.at[part, :], w_buf.at[part, :], sem.at[c]))
    for copy in copies[:AHEAD]:
        copy.start()
    for copy in first_copies:
        copy.wait()
    x = hidden_ref[...].astype(F32)
    mean_square = jnp.sum(x * x, axis=-1, keepdims=True) / depth
    gain = gain_ref[...].reshape(1, depth)
    n_ref[...] = (x * lax.rsqrt(mean_square + 1e-06) * gain).astype(BF16)
    first = lax.axis_index("seq") * rows
    row = row_iota(rows)
    lane = lane_iota(rows)
    length = jnp.zeros((rows, LANES), jnp.int32)
    for i in range(rows):
        length = jnp.where(row == i, lens_ref[first + i], length)
    half = LANES // 2
    low = lane < half
    slot = jnp.where(low, lane, lane - half).astype(F32)
    frequency = jnp.exp(slot * (-9.210340371976184 / half))
    angles = (length + prompt_len).astype(F32) * frequency
    cosine = jnp.cos(angles)
    sines = jnp.sin(angles)
    sines = jnp.where(low, -sines, sines)
    cs_ref[:, :LANES] = cosine
    cs_ref[:, LANES:] = sines
    total = jnp.zeros((rows, width), F32)
    for c in range(len(chunks)):
        copies[c].wait()
        if c + AHEAD < len(chunks):
            copies[c + AHEAD].start()
        total = total + jnp.dot(
            n_ref[:, edges[c] : edges[c + 1]],
            w_buf[edges[c] : edges[c + 1], :],
            preferred_element_type=F32,
        )
    for h in range(width // LANES):
        v = total[:, h * LANES : (h + 1) * LANES]
        q_ref[:, h * LANES : (h + 1) * LANES] = (
            v * cosine + pltpu.roll(v, half, 1) * sines
        ).astype(BF16)


CODE = 256
AHEAD = 4


def plan_kernel(pages, block_len, tasks, table_ref, lens_ref, task_ref, meta_ref):
    blocks, requests = table_ref.shape
    seq = lax.axis_index("seq")
    table = table_ref[...] - seq * pages
    lens = lens_ref[...]
    shape = (blocks, requests)
    block = lax.broadcasted_iota(jnp.int32, shape, 0)
    owner = lax.broadcasted_iota(jnp.int32, shape, 1)
    live = jnp.minimum(lens - block * block_len, block_len)
    code = jnp.where(live > 0, owner * CODE + live, 0)
    columns = []
    for p in range(pages):
        hit = jnp.where(table == p, code, 0)
        fold = hit[:SUB]
        for j in range(1, blocks // SUB):
            fold = fold + hit[j * SUB : (j + 1) * SUB]
        columns.append(jnp.sum(fold.astype(F32), axis=0, keepdims=True))
    found = jnp.sum(jnp.concatenate(columns, axis=0), axis=1, keepdims=True)
    at = lane_iota(pages) == row_iota(pages)
    first = jnp.sum(jnp.where(at, found, 0.0), axis=0, keepdims=True)
    task = task_ref[...] - seq * tasks
    here = (task >= 0) & (task < tasks)
    flag = jnp.broadcast_to(here.astype(F32), (SUB, requests))
    before = (
        lax.broadcasted_iota(jnp.int32, (requests, requests), 0)
        < lax.broadcasted_iota(jnp.int32, (requests, requests), 1)
    )
    rank = jnp.dot(flag.astype(BF16), before.astype(F32).astype(BF16), preferred_element_type=F32)[:1]
    item = lax.broadcasted_iota(jnp.int32, (requests, requests), 0)
    column = lax.broadcasted_iota(jnp.int32, (1, requests), 1)
    entry = (column * CODE + task).astype(F32)
    pick = (rank.astype(jnp.int32) == item) & here
    listed = jnp.sum(jnp.where(pick, entry, 0.0), axis=1, keepdims=True)
    same = item == lax.broadcasted_iota(jnp.int32, (requests, requests), 1)
    second = jnp.sum(jnp.where(same, listed, 0.0), axis=0, keepdims=True)
    count = jnp.sum(flag[:1], axis=1, keepdims=True)
    third = jnp.broadcast_to(count, (1, requests))
    rest = jnp.zeros((SUB - 3, requests), F32)
    meta_ref[...] = jnp.concatenate([first, second, third, rest], axis=0).astype(jnp.int32)


def attend_kernel(
    n_seq, score_scale, batch,
    meta_hbm, q_refs, pages_ref, prompt_ref, own_ref, near_ref, msg_ref, meta_ref, qf, acc, acw, sem,
):
    rows, width = q_refs[0].shape
    heads = width // LANES
    pages, _, block_len, kv_width = pages_ref.shape
    kvh = kv_width // LANES
    group = heads // kvh
    prompt_len = prompt_ref.shape[2]
    me = lax.axis_index("seq")
    fetch = pltpu.make_async_copy(meta_hbm, meta_ref, sem)
    fetch.start()
    acc[...] = jnp.zeros_like(acc)
    acw[...] = jnp.zeros_like(acw)
    for k in range(n_seq):
        base = pl.multiple_of((me ^ k) * (rows * heads), SUB)
        for h in range(heads):
            qf[pl.ds(base + h, rows, stride=heads), :] = q_refs[k][
                :, h * LANES : (h + 1) * LANES
            ].astype(F32)
    fetch.wait()
    sub = row_iota(heads) // group
    lane = lane_iota(heads)
    zero = jnp.zeros((heads, LANES), F32)

    def spread(r):
        q = qf[pl.ds(pl.multiple_of(r * heads, SUB), heads), :]
        return jnp.concatenate([jnp.where(sub == g, q, zero) for g in range(kvh)], axis=1)

    def weigh(s, live):
        w = jnp.exp(cap_limit * jnp.tanh(s * (score_scale / cap_limit)))
        return jnp.where(live, w, zero)

    def collect(o):
        out = zero
        for g in range(kvh):
            out = jnp.where(sub == g, o[:, g * LANES : (g + 1) * LANES], out)
        return out

    def add(r, w, o):
        at = pl.ds(pl.multiple_of(r * heads, SUB), heads)
        acw[at, :] = acw[at, :] + w
        acc[at, :] = acc[at, :] + o

    pair = 2

    def page_step(i, c):
        owners, weights, values = [], [], []
        for b in range(batch):
            p = (i * batch + b) * pair
            note = [meta_ref[0, p + j] for j in range(pair)]
            who = [n // CODE for n in note]
            q2 = jnp.concatenate([spread(r) for r in who], axis=0).astype(BF16)
            keys = pages_ref[pl.ds(p, pair), 0].reshape(pair * block_len, kv_width)
            s = lax.dot_general(q2, keys, (((1,), (1,)), ((), ())), preferred_element_type=F32)
            ws = []
            for j in range(pair):
                live = lane < note[j] % CODE
                ws.append(weigh(s[j * heads : (j + 1) * heads, j * block_len : (j + 1) * block_len], live))
            owners.append(who)
            weights.append(ws)
        for b in range(batch):
            p = (i * batch + b) * pair
            ws = weights[b]
            w2 = jnp.concatenate(
                [
                    jnp.concatenate([ws[j] if m == j else zero for m in range(pair)], axis=1)
                    for j in range(pair)
                ],
                axis=0,
            ).astype(BF16)
            vals = pages_ref[pl.ds(p, pair), 1].reshape(pair * block_len, kv_width)
            values.append(jnp.dot(w2, vals, preferred_element_type=F32))
        for b in range(batch):
            for j in range(pair):
                add(owners[b][j], weights[b][j], collect(values[b][j * heads : (j + 1) * heads]))
        return c

    steps = pages // (pair * batch)
    lax.fori_loop(0, steps, page_step, 0)

    count = meta_ref[2, 0]
    per = LANES // prompt_len
    quad = 2 * per
    pbatch = 4

    def prompt_step(i, c):
        owners, weights, values, tasks = [], [], [], []
        for b in range(pbatch):
            e = (i * pbatch + b) * quad
            note = [meta_ref[1, e + j] for j in range(quad)]
            who = [n // CODE for n in note]
            task = [n % CODE for n in note]
            q4 = jnp.concatenate([spread(r) for r in who], axis=0).astype(BF16)
            keys = jnp.concatenate([prompt_ref[t, 0] for t in task], axis=0)
            s = lax.dot_general(q4, keys, (((1,), (1,)), ((), ())), preferred_element_type=F32)
            ws = []
            for j in range(quad):
                tile = j // per
                live = (lane // prompt_len == j % per) & (e + j < count)
                ws.append(weigh(s[j * heads : (j + 1) * heads, tile * LANES : (tile + 1) * LANES], live))
            owners.append(who)
            weights.append(ws)
            tasks.append(task)
        for b in range(pbatch):
            ws = weights[b]
            w4 = jnp.concatenate(
                [
                    jnp.concatenate([ws[j] if m == j // per else zero for m in range(2)], axis=1)
                    for j in range(quad)
                ],
                axis=0,
            ).astype(BF16)
            vals = jnp.concatenate([prompt_ref[t, 1] for t in tasks[b]], axis=0)
            values.append(jnp.dot(w4, vals, preferred_element_type=F32))
        for b in range(pbatch):
            for j in range(quad):
                add(owners[b][j], weights[b][j], collect(values[b][j * heads : (j + 1) * heads]))
        return c

    lax.fori_loop(0, (count + quad * pbatch - 1) // (quad * pbatch), prompt_step, 0)

    lanes = lane_iota(rows)
    for k in range(n_seq):
        base = (me ^ k) * (rows * heads)
        sums = jnp.zeros((rows, LANES), F32)
        out = (own_ref, msg_ref.at[:rows], near_ref, msg_ref.at[rows:])[k]
        for h in range(heads):
            at = pl.ds(base + h, rows, stride=heads)
            out[:, h * LANES : (h + 1) * LANES] = acc[at, :].astype(out.dtype)
            tot = jnp.sum(acw[at, :], axis=1, keepdims=True)
            sums = jnp.where(lanes == h, tot, sums)
        if k % 2:
            sums = two_parts(sums, heads)
        out[:, heads * LANES :] = sums.astype(out.dtype)


def two_parts(sums, heads):
    top = sums.astype(BF16).astype(F32)
    return top + pltpu.roll(sums - top, heads, 1)


def one_part(sums, heads):
    whole = sums + pltpu.roll(sums, LANES - heads, 1)
    return jnp.where(lane_iota(sums.shape[0]) < heads, whole, 0.0)


def merge_kernel(near_ref, msg_ref, out_ref):
    rows, wide = near_ref.shape
    heads = wide // LANES - 1
    for h in range(heads):
        at = slice(h * LANES, (h + 1) * LANES)
        out_ref[:, at] = (near_ref[:, at] + msg_ref[rows:, at].astype(F32)).astype(BF16)
    at = slice(heads * LANES, wide)
    sums = near_ref[:, at] + one_part(msg_ref[rows:, at].astype(F32), heads)
    out_ref[:, at] = two_parts(sums, heads).astype(BF16)


def fresh_kernel(score_scale, n_ref, cs_ref, q_ref, wk_ref, wv_ref, k_ref, v_ref, self_ref):
    rows, width = q_ref.shape
    heads = width // LANES
    kvh = k_ref.shape[1] // LANES
    group = heads // kvh
    half = LANES // 2
    normed = n_ref[...]
    cosine = cs_ref[:, :LANES]
    sines = cs_ref[:, LANES:]
    keys = jnp.dot(normed, wk_ref[...], preferred_element_type=F32)
    values = jnp.dot(normed, wv_ref[...], preferred_element_type=F32)
    lanes = lane_iota(rows)
    sums = jnp.zeros((rows, LANES), F32)
    for g in range(kvh):
        at = slice(g * LANES, (g + 1) * LANES)
        key = keys[:, at]
        key = (key * cosine + pltpu.roll(key, half, 1) * sines).astype(BF16)
        k_ref[:, at] = key
        key = key.astype(F32)
        val = values[:, at].astype(BF16)
        v_ref[:, at] = val
        val = val.astype(F32)
        for j in range(group):
            h = g * group + j
            raw = jnp.sum(q_ref[:, h * LANES : (h + 1) * LANES].astype(F32) * key, axis=1, keepdims=True)
            w = jnp.exp(cap_limit * jnp.tanh(raw * (score_scale / cap_limit)))
            self_ref[:, h * LANES : (h + 1) * LANES] = w.astype(BF16).astype(F32) * val
            sums = jnp.where(lanes == h, w, sums)
    self_ref[:, heads * LANES :] = sums


def blend_kernel(n_ten, w_ref, own_ref, self_ref, msg_ref, got_ref, att_ref, *out_refs):
    rows, wide = own_ref.shape
    heads = wide // LANES - 1
    at = slice(heads * LANES, wide)
    sums = own_ref[:, at] + self_ref[:, at]
    sums = sums + one_part(msg_ref[:rows, at].astype(F32) + got_ref[:, at].astype(F32), heads)
    for h in range(heads):
        at = slice(h * LANES, (h + 1) * LANES)
        mix = own_ref[:, at] + self_ref[:, at]
        mix = mix + msg_ref[:rows, at].astype(F32) + got_ref[:, at].astype(F32)
        att_ref[:, at] = (mix / sums[:, h : h + 1]).astype(BF16)
    for i, out_ref in enumerate(out_refs):
        project_part(n_ten - 1 - i, att_ref, w_ref, out_ref)


def project_part(k, att_ref, w_ref, out_ref):
    cols = out_ref.shape[1]
    start = pl.multiple_of((lax.axis_index("tensor") ^ k) * cols, LANES)
    got = jnp.dot(att_ref[...], w_ref[:, pl.ds(start, cols)], preferred_element_type=F32)
    out_ref[...] = got.astype(out_ref.dtype)


def project_kernel(w_ref, att_ref, *out_refs):
    for k, out_ref in enumerate(out_refs):
        project_part(k, att_ref, w_ref, out_ref)


def sum_kernel(p0_ref, got_refs, sum_ref, sq_ref):
    rows, cols = p0_ref.shape
    sq = jnp.zeros((rows, LANES), F32)
    for c in range(cols // LANES):
        at = slice(c * LANES, (c + 1) * LANES)
        t = p0_ref[:, at]
        for r in got_refs:
            t = t + r[:, at].astype(F32)
        sum_ref[:, at] = t
        sq = sq + t * t
    sq_ref[...] = sq


def last_kernel(sum_ref, sq_ref, got_refs, hidden_ref, gain_ref, out_ref):
    cols = out_ref.shape[1]
    sq = sq_ref[...]
    for r in got_refs:
        sq = sq + r[...]
    mean_square = jnp.sum(sq, axis=1, keepdims=True) / hidden_ref.shape[1]
    start = pl.multiple_of(lax.axis_index("tensor") * cols, LANES)
    residual = hidden_ref[:, pl.ds(start, cols)].astype(F32)
    out_ref[...] = (
        residual + sum_ref[...] * lax.rsqrt(mean_square + 1e-06) * gain_ref[...]
    ).astype(BF16)


def params(mib):
    return pltpu.CompilerParams(vmem_limit_bytes=mib << 20)


def swap(array, axis, size, k):
    return lax.ppermute(array, axis, [(i, i ^ k) for i in range(size)])


def split(depth, count):
    unit = 2 * LANES
    step = max(1, depth // (unit * count)) * unit
    edges = list(range(0, depth - step + 1, step)) + [depth]
    return tuple(b - a for a, b in zip(edges, edges[1:]))


def in_hbm(array):
    return pltpu.with_memory_space_constraint(array, pltpu.HBM)


def shape(dims, dtype):
    return jax.ShapeDtypeStruct(dims, dtype)


def fast_body(
    n_seq,
    n_ten,
    hidden,
    pre_gain,
    w_query,
    w_key,
    w_value,
    w_out,
    post_gain,
    cache_pool,
    prompt_cache,
    task_ids,
    cache_lengths,
    block_table,
):
    rows, depth = hidden.shape
    width = w_query.shape[1]
    kv_width = w_key.shape[1]
    heads = width // LANES
    pages, _, block_len, _ = cache_pool.shape
    tasks, _, prompt_len, _ = prompt_cache.shape
    requests = task_ids.shape[0]
    cols = post_gain.shape[0]
    wide = width + LANES
    score_scale = float(D // H) ** (-0.5)
    chunks = split(depth, 6)
    query, normed, cs = pl.pallas_call(
        functools.partial(query_kernel, prompt_len, chunks),
        out_shape=(
            pltpu.VMEM((rows, width), BF16),
            pltpu.VMEM((rows, depth), BF16),
            pltpu.VMEM((rows, 2 * LANES), F32),
        ),
        in_specs=[HB] * 4,
        out_specs=(VM, VM, VM),
        scratch_shapes=[
            pltpu.SMEM((requests,), jnp.int32),
            pltpu.VMEM((rows, depth), BF16),
            pltpu.VMEM((depth,), F32),
            pltpu.VMEM((depth, width), BF16),
            pltpu.SemaphoreType.DMA((len(chunks),)),
            pltpu.SemaphoreType.DMA((3,)),
        ],
        compiler_params=params(Q_MIB),
        cost_estimate=cost(0.05),
        name="query",
    )(*[in_hbm(a) for a in (cache_lengths, hidden, pre_gain, w_query)])
    query = pl.pallas_call(
        lambda q, o: None,
        out_shape=pltpu.VMEM((rows, width), BF16),
        in_specs=[VM],
        out_specs=VM,
        input_output_aliases={0: 0},
        compiler_params=params(1),
        cost_estimate=cost(12),
        name="gate",
    )(query)
    near = swap(query, "seq", n_seq, 2)
    side = swap(query, "seq", n_seq, 1)
    far = swap(near, "seq", n_seq, 1)
    meta = pl.pallas_call(
        functools.partial(plan_kernel, pages, block_len, tasks),
        out_shape=shape((SUB, requests), jnp.int32),
        in_specs=[VM, VM, VM],
        out_specs=VM,
        compiler_params=params(1),
        cost_estimate=cost(0.3),
        name="plan",
    )(block_table.T, cache_lengths.reshape(1, requests), task_ids.reshape(1, requests))
    batch = pages // 2
    own, near, msg = pl.pallas_call(
        lambda meta_r, q0, q1, q2, q3, *rest: attend_kernel(
            n_seq, score_scale, batch, meta_r, (q0, q1, q2, q3), *rest
        ),
        out_shape=(
            shape((rows, wide), F32),
            shape((rows, wide), F32),
            shape((2 * rows, wide), BF16),
        ),
        in_specs=[HB] + [VM] * (n_seq + 2),
        out_specs=(VM,) * 3,
        scratch_shapes=[
            pltpu.SMEM((SUB, requests), jnp.int32),
            pltpu.VMEM((requests * heads, LANES), F32),
            pltpu.VMEM((requests * heads, LANES), F32),
            pltpu.VMEM((requests * heads, LANES), F32),
            pltpu.SemaphoreType.DMA,
        ],
        compiler_params=params(A_MIB),
        cost_estimate=cost(8),
        name="attend",
    )(meta, query, side, near, far, cache_pool, prompt_cache)
    msg = swap(msg, "seq", n_seq, 1)
    merged = pl.pallas_call(
        merge_kernel,
        out_shape=shape((rows, wide), BF16),
        in_specs=[VM] * 2,
        out_specs=VM,
        compiler_params=params(1),
        cost_estimate=cost(0.1),
        name="merge",
    )(near, msg)
    got = swap(merged, "seq", n_seq, 2)
    key_new, value_new, self_part = pl.pallas_call(
        functools.partial(fresh_kernel, score_scale),
        out_shape=(shape((rows, kv_width), BF16), shape((rows, kv_width), BF16), shape((rows, wide), F32)),
        in_specs=[VM] * 5,
        out_specs=(VM,) * 3,
        compiler_params=params(G_MIB),
        cost_estimate=cost(1.7),
        name="fresh",
    )(normed, cs, query, w_key, w_value)
    att, part3, part2 = pl.pallas_call(
        functools.partial(blend_kernel, n_ten),
        out_shape=(shape((rows, width), BF16),) + (shape((rows, cols), BF16),) * 2,
        in_specs=[VM] * 5,
        out_specs=(VM,) * 3,
        compiler_params=params(H_MIB),
        cost_estimate=cost(0.7),
        name="blend",
    )(w_out, own, self_part, msg, got)
    got3 = swap(part3, "tensor", n_ten, 3)
    got2 = swap(part2, "tensor", n_ten, 2)
    p0, part1 = pl.pallas_call(
        project_kernel,
        out_shape=(shape((rows, cols), F32), shape((rows, cols), BF16)),
        in_specs=[VM] * 2,
        out_specs=(VM,) * 2,
        compiler_params=params(H_MIB),
        cost_estimate=cost(1.3),
        name="project",
    )(w_out, att)
    got1 = swap(part1, "tensor", n_ten, 1)
    got = [got1, got2, got3]
    total, sq = pl.pallas_call(
        lambda p0, r1, r2, r3, t, s: sum_kernel(p0, (r1, r2, r3), t, s),
        out_shape=(shape((rows, cols), F32), shape((rows, LANES), F32)),
        in_specs=[VM] * n_ten,
        out_specs=(VM,) * 2,
        compiler_params=params(2),
        cost_estimate=cost(0.3),
        name="sum",
    )(p0, *got)
    got = [swap(sq, "tensor", n_ten, k) for k in (1, 2, 3)]
    layer_out = pl.pallas_call(
        lambda t, s, r1, r2, r3, hd, g, o: last_kernel(t, s, (r1, r2, r3), hd, g, o),
        out_shape=shape((rows, cols), BF16),
        in_specs=[VM] * (n_ten + 3),
        out_specs=VM,
        compiler_params=params(2),
        cost_estimate=cost(0.3),
        name="last",
    )(total, sq, *got, hidden, post_gain.reshape(1, cols))
    fresh_cache = jnp.stack([key_new, value_new], axis=1)
    return (layer_out, fresh_cache)


Q_MIB = 52
A_MIB = 4
G_MIB = 4
H_MIB = 4


def body(n_seq, n_ten, *args):
    hidden, w_query, post_gain, cache_pool, prompt_cache = args[0], args[2], args[6], args[7], args[8]
    fits = (
        n_seq == 4
        and n_ten == 4
        and w_query.shape[1] == SUB * HD
        and post_gain.shape[0] % LANES == 0
        and cache_pool.shape[2] == LANES
        and cache_pool.shape[0] % SUB == 0
        and LANES % prompt_cache.shape[2] == 0
        and prompt_cache.shape[2] % (2 * SUB) == 0
        and args[9].shape[0] == LANES == hidden.shape[0] * n_seq
        and args[11].shape[1] % SUB == 0
        and prompt_cache.shape[0] <= CODE
        and cache_pool.shape[0] <= LANES
        and hidden.shape[0] % (2 * SUB) == 0
    )
    if fits:
        return fast_body(n_seq, n_ten, *args)
    return plain_body(*args)


def solution(mesh):
    return jax.shard_map(
        functools.partial(body, mesh.shape["seq"], mesh.shape["tensor"]),
        mesh=mesh,
        in_specs=(
            P(("groups", "seq"), None),
            P(),
            P(None, "tensor"),
            P(None, "tensor"),
            P(None, "tensor"),
            P("tensor", None),
            P("tensor"),
            P(("groups", "seq"), None, None, "tensor"),
            P("seq", None, None, "tensor"),
            P("groups"),
            P("groups"),
            P("groups", None),
        ),
        out_specs=(P(("groups", "seq"), "tensor"), P(("groups", "seq"), None, "tensor")),
        check_vma=False,
    )
```

```python
import functools

import jax
import jax.numpy as jnp
from jax import lax
from jax.experimental import pallas as pl
from jax.experimental.pallas import tpu as pltpu
from jax.sharding import PartitionSpec as P

D = 4608
H = 32
HD = 128
LANES = 128
SUB = 8

cap_limit = 50.0
FLOPS_US = 1 << 30
BYTES_US = 1 << 20
F32 = jnp.float32
BF16 = jnp.bfloat16


def rms_scale(values, gain):
    mean_square = jnp.mean(values * values, axis=-1, keepdims=True)
    return values * lax.rsqrt(mean_square + 1e-06) * gain


def rotate(values, position):
    half_dim = values.shape[-1] // 2
    frequency = 10000.0 ** (-jnp.arange(half_dim, dtype=jnp.float32) / half_dim)
    angles = position.astype(jnp.float32)[:, None] * frequency[None, :]
    cosine = jnp.cos(angles)[:, None, :]
    sines = jnp.sin(angles)[:, None, :]
    first_half = values[..., :half_dim]
    second_half = values[..., half_dim:]
    return jnp.concatenate(
        [first_half * cosine - second_half * sines, second_half * cosine + first_half * sines],
        axis=-1,
    )


def capped(raw_score, score_scale):
    return cap_limit * jnp.tanh(raw_score * score_scale / cap_limit)


def attend(query_block, block, live_mask, score_scale):
    count = block.shape[0]
    length = block.shape[2]
    kv_heads = query_block.shape[1]
    head_dim = query_block.shape[3]
    block_keys = block[:, 0].reshape(count, length, kv_heads, head_dim)
    block_values = block[:, 1].reshape(count, length, kv_heads, head_dim)
    raw_score = jnp.einsum(
        "nkgd,ntkd->nkgt", query_block, block_keys, preferred_element_type=jnp.float32
    )
    weight = jnp.where(live_mask[:, None, None, :], jnp.exp(capped(raw_score, score_scale)), 0.0)
    totals = jnp.sum(weight, axis=-1).reshape(count, -1)
    mixtures = jnp.einsum(
        "nkgt,ntkd->nkgd",
        weight.astype(jnp.bfloat16),
        block_values,
        preferred_element_type=jnp.float32,
    )
    return (totals, mixtures.reshape(count, -1))


def plain_body(
    hidden,
    pre_gain,
    w_query,
    w_key,
    w_value,
    w_out,
    post_gain,
    cache_pool,
    prompt_cache,
    task_ids,
    cache_lengths,
    block_table,
):
    seq_index = lax.axis_index("seq")
    tensor_index = lax.axis_index("tensor")
    own_rows = hidden.shape[0]
    requests = task_ids.shape[0]
    pages_dev = cache_pool.shape[0]
    block_len = cache_pool.shape[2]
    kv_width = cache_pool.shape[3]
    head_dim = HD
    kv_heads = kv_width // head_dim
    query_heads = w_query.shape[1] // head_dim
    group_size = query_heads // kv_heads
    prompt_len = prompt_cache.shape[2]
    tasks_dev = prompt_cache.shape[0]
    score_scale = float(D // H) ** (-0.5)
    first_row = seq_index * own_rows
    own_lengths = lax.dynamic_slice_in_dim(cache_lengths, first_row, own_rows)
    normed = rms_scale(hidden.astype(jnp.float32), pre_gain).astype(jnp.bfloat16)
    position = prompt_len + own_lengths
    query_rows = rotate(
        jnp.dot(normed, w_query, preferred_element_type=jnp.float32).reshape(
            own_rows, query_heads, head_dim
        ),
        position,
    ).astype(jnp.bfloat16)
    key_new = rotate(
        jnp.dot(normed, w_key, preferred_element_type=jnp.float32).reshape(
            own_rows, kv_heads, head_dim
        ),
        position,
    ).astype(jnp.bfloat16)
    value_new = jnp.dot(normed, w_value, preferred_element_type=jnp.float32).astype(jnp.bfloat16)
    fresh_cache = jnp.stack([key_new.reshape(own_rows, kv_width), value_new], axis=1)
    queries = lax.all_gather(
        query_rows.reshape(own_rows, query_heads * head_dim), "seq", axis=0, tiled=True
    )
    page_ids = seq_index * pages_dev + jnp.arange(pages_dev)
    flat_table = block_table.reshape(-1)
    max_blocks = block_table.shape[1]
    matches = flat_table[None, :] == page_ids[:, None]
    entry_index = jnp.arange(flat_table.shape[0])
    page_used = jnp.any(matches, axis=1)
    found_entry = jnp.sum(jnp.where(matches, entry_index[None, :], 0), axis=1)
    page_owner = found_entry // max_blocks
    block_number = found_entry % max_blocks
    owner_hot = (page_owner[:, None] == jnp.arange(requests)[None, :]) & page_used[:, None]
    owner_length = jnp.sum(jnp.where(owner_hot, cache_lengths[None, :], 0), axis=1)
    valid_count = jnp.clip(owner_length - block_number * block_len, 0, block_len)
    page_query = jnp.dot(
        owner_hot.astype(jnp.bfloat16), queries, preferred_element_type=jnp.float32
    ).astype(jnp.bfloat16)
    page_query = page_query.reshape(pages_dev, kv_heads, group_size, head_dim)
    page_live = jnp.arange(block_len)[None, :] < valid_count[:, None]
    page_totals, page_mixtures = attend(page_query, cache_pool, page_live, score_scale)
    spread_hot = owner_hot.astype(jnp.float32).T
    totals = jnp.dot(spread_hot, page_totals, precision=lax.Precision.HIGHEST)
    mixtures = jnp.dot(spread_hot, page_mixtures, precision=lax.Precision.HIGHEST)
    local_task = task_ids - seq_index * tasks_dev
    is_owned = (local_task >= 0) & (local_task < tasks_dev)
    task_rows = prompt_cache[jnp.clip(local_task, 0, tasks_dev - 1)]
    all_query = queries.reshape(requests, kv_heads, group_size, head_dim)
    owned_live = jnp.broadcast_to(is_owned[:, None], (requests, prompt_len))
    prompt_totals, prompt_mixtures = attend(all_query, task_rows, owned_live, score_scale)
    totals = totals + prompt_totals
    mixtures = mixtures + prompt_mixtures
    totals, mixtures = (
        lax.psum_scatter(
            totals.astype(jnp.bfloat16), "seq", scatter_dimension=0, tiled=True
        ).astype(jnp.float32),
        lax.psum_scatter(
            mixtures.astype(jnp.bfloat16), "seq", scatter_dimension=0, tiled=True
        ).astype(jnp.float32),
    )
    own_query = query_rows.reshape(own_rows, kv_heads, group_size, head_dim)
    self_raw = jnp.sum(
        own_query.astype(jnp.float32) * key_new[:, :, None, :].astype(jnp.float32), axis=-1
    )
    self_weight = jnp.exp(capped(self_raw, score_scale))
    rounded = lax.optimization_barrier(self_weight.astype(jnp.bfloat16)).astype(jnp.float32)
    totals = totals + self_weight.reshape(own_rows, -1)
    self_mix = rounded[..., None] * value_new.reshape(own_rows, kv_heads, 1, head_dim).astype(
        jnp.float32
    )
    mixtures = mixtures + self_mix.reshape(own_rows, -1)
    attended = (mixtures.reshape(own_rows, query_heads, head_dim) / totals[..., None]).astype(
        jnp.bfloat16
    )
    projected = jnp.dot(
        attended.reshape(own_rows, query_heads * head_dim),
        w_out,
        preferred_element_type=jnp.float32,
    )
    cols_local = post_gain.shape[0]
    col_start = tensor_index * cols_local
    residual = lax.dynamic_slice_in_dim(hidden, col_start, cols_local, 1).astype(jnp.float32)
    whole_sum = lax.psum(projected.astype(jnp.bfloat16), "tensor").astype(jnp.float32)
    mean_square = jnp.mean(whole_sum * whole_sum, axis=1, keepdims=True)
    scaled = lax.dynamic_slice_in_dim(whole_sum, col_start, cols_local, 1) * lax.rsqrt(
        mean_square + 1e-06
    )
    layer_out = (residual + scaled * post_gain).astype(jnp.bfloat16)
    return (layer_out, fresh_cache)


VM = pl.BlockSpec(memory_space=pltpu.VMEM)
SM = pl.BlockSpec(memory_space=pltpu.SMEM)
HB = pl.BlockSpec(memory_space=pltpu.HBM)


def cost(us):
    return pl.CostEstimate(
        flops=int(us * FLOPS_US), bytes_accessed=int(us * BYTES_US), transcendentals=0
    )


def row_iota(rows):
    return lax.broadcasted_iota(jnp.int32, (rows, LANES), 0)


def lane_iota(rows):
    return lax.broadcasted_iota(jnp.int32, (rows, LANES), 1)


def query_kernel(
    prompt_len, chunks, lens_hbm, hidden_hbm, gain_hbm, w_ref, q_ref, n_ref, cs_ref,
    lens_ref, hidden_ref, gain_ref, w_buf, sem, small,
):
    rows, depth = hidden_ref.shape
    width = q_ref.shape[1]
    edges = [0]
    for c in chunks:
        edges.append(edges[-1] + c)
    first_copies = [
        pltpu.make_async_copy(hidden_hbm, hidden_ref, small.at[0]),
        pltpu.make_async_copy(gain_hbm, gain_ref, small.at[1]),
        pltpu.make_async_copy(lens_hbm, lens_ref, small.at[2]),
    ]
    for copy in first_copies:
        copy.start()
    copies = []
    for c in range(len(chunks)):
        part = pl.ds(edges[c], chunks[c])
        copies.append(pltpu.make_async_copy(w_ref.at[part, :], w_buf.at[part, :], sem.at[c]))
    for copy in copies[:AHEAD]:
        copy.start()
    for copy in first_copies:
        copy.wait()
    x = hidden_ref[...].astype(F32)
    mean_square = jnp.sum(x * x, axis=-1, keepdims=True) / depth
    gain = gain_ref[...].reshape(1, depth)
    n_ref[...] = (x * lax.rsqrt(mean_square + 1e-06) * gain).astype(BF16)
    first = lax.axis_index("seq") * rows
    row = row_iota(rows)
    lane = lane_iota(rows)
    length = jnp.zeros((rows, LANES), jnp.int32)
    for i in range(rows):
        length = jnp.where(row == i, lens_ref[first + i], length)
    half = LANES // 2
    low = lane < half
    slot = jnp.where(low, lane, lane - half).astype(F32)
    frequency = jnp.exp(slot * (-9.210340371976184 / half))
    angles = (length + prompt_len).astype(F32) * frequency
    cosine = jnp.cos(angles)
    sines = jnp.sin(angles)
    sines = jnp.where(low, -sines, sines)
    cs_ref[:, :LANES] = cosine
    cs_ref[:, LANES:] = sines
    total = jnp.zeros((rows, width), F32)
    for c in range(len(chunks)):
        copies[c].wait()
        if c + AHEAD < len(chunks):
            copies[c + AHEAD].start()
        total = total + jnp.dot(
            n_ref[:, edges[c] : edges[c + 1]],
            w_buf[edges[c] : edges[c + 1], :],
            preferred_element_type=F32,
        )
    for h in range(width // LANES):
        v = total[:, h * LANES : (h + 1) * LANES]
        q_ref[:, h * LANES : (h + 1) * LANES] = (
            v * cosine + pltpu.roll(v, half, 1) * sines
        ).astype(BF16)


CODE = 256
AHEAD = 4


def plan_kernel(pages, block_len, tasks, table_ref, lens_ref, task_ref, meta_ref):
    blocks, requests = table_ref.shape
    seq = lax.axis_index("seq")
    table = table_ref[...] - seq * pages
    lens = lens_ref[...]
    shape = (blocks, requests)
    block = lax.broadcasted_iota(jnp.int32, shape, 0)
    owner = lax.broadcasted_iota(jnp.int32, shape, 1)
    live = jnp.minimum(lens - block * block_len, block_len)
    code = jnp.where(live > 0, owner * CODE + live, 0)
    columns = []
    for p in range(pages):
        hit = jnp.where(table == p, code, 0)
        fold = hit[:SUB]
        for j in range(1, blocks // SUB):
            fold = fold + hit[j * SUB : (j + 1) * SUB]
        columns.append(jnp.sum(fold.astype(F32), axis=0, keepdims=True))
    found = jnp.sum(jnp.concatenate(columns, axis=0), axis=1, keepdims=True)
    at = lane_iota(pages) == row_iota(pages)
    first = jnp.sum(jnp.where(at, found, 0.0), axis=0, keepdims=True)
    task = task_ref[...] - seq * tasks
    here = (task >= 0) & (task < tasks)
    flag = jnp.broadcast_to(here.astype(F32), (SUB, requests))
    before = (
        lax.broadcasted_iota(jnp.int32, (requests, requests), 0)
        < lax.broadcasted_iota(jnp.int32, (requests, requests), 1)
    )
    rank = jnp.dot(flag.astype(BF16), before.astype(F32).astype(BF16), preferred_element_type=F32)[:1]
    item = lax.broadcasted_iota(jnp.int32, (requests, requests), 0)
    column = lax.broadcasted_iota(jnp.int32, (1, requests), 1)
    entry = (column * CODE + task).astype(F32)
    pick = (rank.astype(jnp.int32) == item) & here
    listed = jnp.sum(jnp.where(pick, entry, 0.0), axis=1, keepdims=True)
    same = item == lax.broadcasted_iota(jnp.int32, (requests, requests), 1)
    second = jnp.sum(jnp.where(same, listed, 0.0), axis=0, keepdims=True)
    count = jnp.sum(flag[:1], axis=1, keepdims=True)
    third = jnp.broadcast_to(count, (1, requests))
    rest = jnp.zeros((SUB - 3, requests), F32)
    meta_ref[...] = jnp.concatenate([first, second, third, rest], axis=0).astype(jnp.int32)


def attend_kernel(
    n_seq, score_scale, batch,
    meta_hbm, q_refs, pages_ref, prompt_ref, own_ref, near_ref, msg_ref, meta_ref, qf, acc, acw, sem,
):
    rows, width = q_refs[0].shape
    heads = width // LANES
    pages, _, block_len, kv_width = pages_ref.shape
    kvh = kv_width // LANES
    group = heads // kvh
    prompt_len = prompt_ref.shape[2]
    me = lax.axis_index("seq")
    fetch = pltpu.make_async_copy(meta_hbm, meta_ref, sem)
    fetch.start()
    acc[...] = jnp.zeros_like(acc)
    acw[...] = jnp.zeros_like(acw)
    for k in range(n_seq):
        base = pl.multiple_of((me ^ k) * (rows * heads), SUB)
        for h in range(heads):
            qf[pl.ds(base + h, rows, stride=heads), :] = q_refs[k][
                :, h * LANES : (h + 1) * LANES
            ].astype(F32)
    fetch.wait()
    sub = row_iota(heads) // group
    lane = lane_iota(heads)
    zero = jnp.zeros((heads, LANES), F32)

    def spread(r):
        q = qf[pl.ds(pl.multiple_of(r * heads, SUB), heads), :]
        return jnp.concatenate([jnp.where(sub == g, q, zero) for g in range(kvh)], axis=1)

    def weigh(s, live):
        w = jnp.exp(cap_limit * jnp.tanh(s * (score_scale / cap_limit)))
        return jnp.where(live, w, zero)

    def collect(o):
        out = zero
        for g in range(kvh):
            out = jnp.where(sub == g, o[:, g * LANES : (g + 1) * LANES], out)
        return out

    def add(r, w, o):
        at = pl.ds(pl.multiple_of(r * heads, SUB), heads)
        acw[at, :] = acw[at, :] + w
        acc[at, :] = acc[at, :] + o

    pair = 2

    def page_step(i, c):
        owners, weights, values = [], [], []
        for b in range(batch):
            p = (i * batch + b) * pair
            note = [meta_ref[0, p + j] for j in range(pair)]
            who = [n // CODE for n in note]
            q2 = jnp.concatenate([spread(r) for r in who], axis=0).astype(BF16)
            keys = pages_ref[pl.ds(p, pair), 0].reshape(pair * block_len, kv_width)
            s = lax.dot_general(q2, keys, (((1,), (1,)), ((), ())), preferred_element_type=F32)
            ws = []
            for j in range(pair):
                live = lane < note[j] % CODE
                ws.append(weigh(s[j * heads : (j + 1) * heads, j * block_len : (j + 1) * block_len], live))
            owners.append(who)
            weights.append(ws)
        for b in range(batch):
            p = (i * batch + b) * pair
            ws = weights[b]
            w2 = jnp.concatenate(
                [
                    jnp.concatenate([ws[j] if m == j else zero for m in range(pair)], axis=1)
                    for j in range(pair)
                ],
                axis=0,
            ).astype(BF16)
            vals = pages_ref[pl.ds(p, pair), 1].reshape(pair * block_len, kv_width)
            values.append(jnp.dot(w2, vals, preferred_element_type=F32))
        for b in range(batch):
            for j in range(pair):
                add(owners[b][j], weights[b][j], collect(values[b][j * heads : (j + 1) * heads]))
        return c

    steps = pages // (pair * batch)
    lax.fori_loop(0, steps, page_step, 0)

    count = meta_ref[2, 0]
    per = LANES // prompt_len
    quad = 2 * per
    pbatch = 4

    def prompt_step(i, c):
        owners, weights, values, tasks = [], [], [], []
        for b in range(pbatch):
            e = (i * pbatch + b) * quad
            note = [meta_ref[1, e + j] for j in range(quad)]
            who = [n // CODE for n in note]
            task = [n % CODE for n in note]
            q4 = jnp.concatenate([spread(r) for r in who], axis=0).astype(BF16)
            keys = jnp.concatenate([prompt_ref[t, 0] for t in task], axis=0)
            s = lax.dot_general(q4, keys, (((1,), (1,)), ((), ())), preferred_element_type=F32)
            ws = []
            for j in range(quad):
                tile = j // per
                live = (lane // prompt_len == j % per) & (e + j < count)
                ws.append(weigh(s[j * heads : (j + 1) * heads, tile * LANES : (tile + 1) * LANES], live))
            owners.append(who)
            weights.append(ws)
            tasks.append(task)
        for b in range(pbatch):
            ws = weights[b]
            w4 = jnp.concatenate(
                [
                    jnp.concatenate([ws[j] if m == j // per else zero for m in range(2)], axis=1)
                    for j in range(quad)
                ],
                axis=0,
            ).astype(BF16)
            vals = jnp.concatenate([prompt_ref[t, 1] for t in tasks[b]], axis=0)
            values.append(jnp.dot(w4, vals, preferred_element_type=F32))
        for b in range(pbatch):
            for j in range(quad):
                add(owners[b][j], weights[b][j], collect(values[b][j * heads : (j + 1) * heads]))
        return c

    lax.fori_loop(0, (count + quad * pbatch - 1) // (quad * pbatch), prompt_step, 0)

    lanes = lane_iota(rows)
    for k in range(n_seq):
        base = (me ^ k) * (rows * heads)
        sums = jnp.zeros((rows, LANES), F32)
        out = (own_ref, msg_ref.at[:rows], near_ref, msg_ref.at[rows:])[k]
        for h in range(heads):
            at = pl.ds(base + h, rows, stride=heads)
            out[:, h * LANES : (h + 1) * LANES] = acc[at, :].astype(out.dtype)
            tot = jnp.sum(acw[at, :], axis=1, keepdims=True)
            sums = jnp.where(lanes == h, tot, sums)
        if k % 2:
            sums = two_parts(sums, heads)
        out[:, heads * LANES :] = sums.astype(out.dtype)


def two_parts(sums, heads):
    top = sums.astype(BF16).astype(F32)
    return top + pltpu.roll(sums - top, heads, 1)


def one_part(sums, heads):
    whole = sums + pltpu.roll(sums, LANES - heads, 1)
    return jnp.where(lane_iota(sums.shape[0]) < heads, whole, 0.0)


def merge_kernel(near_ref, msg_ref, out_ref):
    rows, wide = near_ref.shape
    heads = wide // LANES - 1
    for h in range(heads):
        at = slice(h * LANES, (h + 1) * LANES)
        out_ref[:, at] = (near_ref[:, at] + msg_ref[rows:, at].astype(F32)).astype(BF16)
    at = slice(heads * LANES, wide)
    sums = near_ref[:, at] + one_part(msg_ref[rows:, at].astype(F32), heads)
    out_ref[:, at] = two_parts(sums, heads).astype(BF16)


def fresh_kernel(score_scale, n_ref, cs_ref, q_ref, wk_ref, wv_ref, k_ref, v_ref, self_ref):
    rows, width = q_ref.shape
    heads = width // LANES
    kvh = k_ref.shape[1] // LANES
    group = heads // kvh
    half = LANES // 2
    normed = n_ref[...]
    cosine = cs_ref[:, :LANES]
    sines = cs_ref[:, LANES:]
    keys = jnp.dot(normed, wk_ref[...], preferred_element_type=F32)
    values = jnp.dot(normed, wv_ref[...], preferred_element_type=F32)
    lanes = lane_iota(rows)
    sums = jnp.zeros((rows, LANES), F32)
    for g in range(kvh):
        at = slice(g * LANES, (g + 1) * LANES)
        key = keys[:, at]
        key = (key * cosine + pltpu.roll(key, half, 1) * sines).astype(BF16)
        k_ref[:, at] = key
        key = key.astype(F32)
        val = values[:, at].astype(BF16)
        v_ref[:, at] = val
        val = val.astype(F32)
        for j in range(group):
            h = g * group + j
            raw = jnp.sum(q_ref[:, h * LANES : (h + 1) * LANES].astype(F32) * key, axis=1, keepdims=True)
            w = jnp.exp(cap_limit * jnp.tanh(raw * (score_scale / cap_limit)))
            self_ref[:, h * LANES : (h + 1) * LANES] = w.astype(BF16).astype(F32) * val
            sums = jnp.where(lanes == h, w, sums)
    self_ref[:, heads * LANES :] = sums


def blend_kernel(n_ten, w_ref, own_ref, self_ref, msg_ref, got_ref, att_ref, *out_refs):
    rows, wide = own_ref.shape
    heads = wide // LANES - 1
    at = slice(heads * LANES, wide)
    sums = own_ref[:, at] + self_ref[:, at]
    sums = sums + one_part(msg_ref[:rows, at].astype(F32) + got_ref[:, at].astype(F32), heads)
    for h in range(heads):
        at = slice(h * LANES, (h + 1) * LANES)
        mix = own_ref[:, at] + self_ref[:, at]
        mix = mix + msg_ref[:rows, at].astype(F32) + got_ref[:, at].astype(F32)
        att_ref[:, at] = (mix / sums[:, h : h + 1]).astype(BF16)
    for i, out_ref in enumerate(out_refs):
        project_part(n_ten - 1 - i, att_ref, w_ref, out_ref)


def project_part(k, att_ref, w_ref, out_ref):
    cols = out_ref.shape[1]
    start = pl.multiple_of((lax.axis_index("tensor") ^ k) * cols, LANES)
    got = jnp.dot(att_ref[...], w_ref[:, pl.ds(start, cols)], preferred_element_type=F32)
    out_ref[...] = got.astype(out_ref.dtype)


def project_kernel(w_ref, att_ref, *out_refs):
    for k, out_ref in enumerate(out_refs):
        project_part(k, att_ref, w_ref, out_ref)


def sum_kernel(p0_ref, got_refs, sum_ref, sq_ref):
    rows, cols = p0_ref.shape
    sq = jnp.zeros((rows, LANES), F32)
    for c in range(cols // LANES):
        at = slice(c * LANES, (c + 1) * LANES)
        t = p0_ref[:, at]
        for r in got_refs:
            t = t + r[:, at].astype(F32)
        sum_ref[:, at] = t
        sq = sq + t * t
    sq_ref[...] = sq


def last_kernel(sum_ref, sq_ref, got_refs, hidden_ref, gain_ref, out_ref):
    cols = out_ref.shape[1]
    sq = sq_ref[...]
    for r in got_refs:
        sq = sq + r[...]
    mean_square = jnp.sum(sq, axis=1, keepdims=True) / hidden_ref.shape[1]
    start = pl.multiple_of(lax.axis_index("tensor") * cols, LANES)
    residual = hidden_ref[:, pl.ds(start, cols)].astype(F32)
    out_ref[...] = (
        residual + sum_ref[...] * lax.rsqrt(mean_square + 1e-06) * gain_ref[...]
    ).astype(BF16)


def params(mib):
    return pltpu.CompilerParams(vmem_limit_bytes=mib << 20)


def swap(array, axis, size, k):
    return lax.ppermute(array, axis, [(i, i ^ k) for i in range(size)])


def split(depth, count):
    unit = 2 * LANES
    step = max(1, depth // (unit * count)) * unit
    edges = list(range(0, depth - step + 1, step)) + [depth]
    return tuple(b - a for a, b in zip(edges, edges[1:]))


def in_hbm(array):
    return pltpu.with_memory_space_constraint(array, pltpu.HBM)


def shape(dims, dtype):
    return jax.ShapeDtypeStruct(dims, dtype)


def fast_body(
    n_seq,
    n_ten,
    hidden,
    pre_gain,
    w_query,
    w_key,
    w_value,
    w_out,
    post_gain,
    cache_pool,
    prompt_cache,
    task_ids,
    cache_lengths,
    block_table,
):
    rows, depth = hidden.shape
    width = w_query.shape[1]
    kv_width = w_key.shape[1]
    heads = width // LANES
    pages, _, block_len, _ = cache_pool.shape
    tasks, _, prompt_len, _ = prompt_cache.shape
    requests = task_ids.shape[0]
    cols = post_gain.shape[0]
    wide = width + LANES
    score_scale = float(D // H) ** (-0.5)
    chunks = split(depth, 6)
    query, normed, cs = pl.pallas_call(
        functools.partial(query_kernel, prompt_len, chunks),
        out_shape=(
            pltpu.VMEM((rows, width), BF16),
            pltpu.VMEM((rows, depth), BF16),
            pltpu.VMEM((rows, 2 * LANES), F32),
        ),
        in_specs=[HB] * 4,
        out_specs=(VM, VM, VM),
        scratch_shapes=[
            pltpu.SMEM((requests,), jnp.int32),
            pltpu.VMEM((rows, depth), BF16),
            pltpu.VMEM((depth,), F32),
            pltpu.VMEM((depth, width), BF16),
            pltpu.SemaphoreType.DMA((len(chunks),)),
            pltpu.SemaphoreType.DMA((3,)),
        ],
        compiler_params=params(Q_MIB),
        cost_estimate=cost(4),
        name="query",
    )(*[in_hbm(a) for a in (cache_lengths, hidden, pre_gain, w_query)])
    query = pl.pallas_call(
        lambda q, o: None,
        out_shape=pltpu.VMEM((rows, width), BF16),
        in_specs=[VM],
        out_specs=VM,
        input_output_aliases={0: 0},
        compiler_params=params(1),
        cost_estimate=cost(5),
        name="gate",
    )(query)
    near = swap(query, "seq", n_seq, 2)
    side = swap(query, "seq", n_seq, 1)
    far = swap(near, "seq", n_seq, 1)
    meta = pl.pallas_call(
        functools.partial(plan_kernel, pages, block_len, tasks),
        out_shape=shape((SUB, requests), jnp.int32),
        in_specs=[VM, VM, VM],
        out_specs=VM,
        compiler_params=params(1),
        cost_estimate=cost(0.3),
        name="plan",
    )(block_table.T, cache_lengths.reshape(1, requests), task_ids.reshape(1, requests))
    batch = pages // 2
    own, near, msg = pl.pallas_call(
        lambda meta_r, q0, q1, q2, q3, *rest: attend_kernel(
            n_seq, score_scale, batch, meta_r, (q0, q1, q2, q3), *rest
        ),
        out_shape=(
            shape((rows, wide), F32),
            shape((rows, wide), F32),
            shape((2 * rows, wide), BF16),
        ),
        in_specs=[HB] + [VM] * (n_seq + 2),
        out_specs=(VM,) * 3,
        scratch_shapes=[
            pltpu.SMEM((SUB, requests), jnp.int32),
            pltpu.VMEM((requests * heads, LANES), F32),
            pltpu.VMEM((requests * heads, LANES), F32),
            pltpu.VMEM((requests * heads, LANES), F32),
            pltpu.SemaphoreType.DMA,
        ],
        compiler_params=params(A_MIB),
        cost_estimate=cost(8),
        name="attend",
    )(meta, query, side, near, far, cache_pool, prompt_cache)
    msg = swap(msg, "seq", n_seq, 1)
    merged = pl.pallas_call(
        merge_kernel,
        out_shape=shape((rows, wide), BF16),
        in_specs=[VM] * 2,
        out_specs=VM,
        compiler_params=params(1),
        cost_estimate=cost(0.1),
        name="merge",
    )(near, msg)
    got = swap(merged, "seq", n_seq, 2)
    key_new, value_new, self_part = pl.pallas_call(
        functools.partial(fresh_kernel, score_scale),
        out_shape=(shape((rows, kv_width), BF16), shape((rows, kv_width), BF16), shape((rows, wide), F32)),
        in_specs=[VM] * 5,
        out_specs=(VM,) * 3,
        compiler_params=params(G_MIB),
        cost_estimate=cost(1.7),
        name="fresh",
    )(normed, cs, query, w_key, w_value)
    att, part3, part2 = pl.pallas_call(
        functools.partial(blend_kernel, n_ten),
        out_shape=(shape((rows, width), BF16),) + (shape((rows, cols), BF16),) * 2,
        in_specs=[VM] * 5,
        out_specs=(VM,) * 3,
        compiler_params=params(H_MIB),
        cost_estimate=cost(0.7),
        name="blend",
    )(w_out, own, self_part, msg, got)
    got3 = swap(part3, "tensor", n_ten, 3)
    got2 = swap(part2, "tensor", n_ten, 2)
    p0, part1 = pl.pallas_call(
        project_kernel,
        out_shape=(shape((rows, cols), F32), shape((rows, cols), BF16)),
        in_specs=[VM] * 2,
        out_specs=(VM,) * 2,
        compiler_params=params(H_MIB),
        cost_estimate=cost(1.3),
        name="project",
    )(w_out, att)
    got1 = swap(part1, "tensor", n_ten, 1)
    got = [got1, got2, got3]
    total, sq = pl.pallas_call(
        lambda p0, r1, r2, r3, t, s: sum_kernel(p0, (r1, r2, r3), t, s),
        out_shape=(shape((rows, cols), F32), shape((rows, LANES), F32)),
        in_specs=[VM] * n_ten,
        out_specs=(VM,) * 2,
        compiler_params=params(2),
        cost_estimate=cost(0.3),
        name="sum",
    )(p0, *got)
    got = [swap(sq, "tensor", n_ten, k) for k in (1, 2, 3)]
    layer_out = pl.pallas_call(
        lambda t, s, r1, r2, r3, hd, g, o: last_kernel(t, s, (r1, r2, r3), hd, g, o),
        out_shape=shape((rows, cols), BF16),
        in_specs=[VM] * (n_ten + 3),
        out_specs=VM,
        compiler_params=params(2),
        cost_estimate=cost(0.3),
        name="last",
    )(total, sq, *got, hidden, post_gain.reshape(1, cols))
    fresh_cache = jnp.stack([key_new, value_new], axis=1)
    return (layer_out, fresh_cache)


Q_MIB = 48
A_MIB = 4
G_MIB = 4
H_MIB = 4


def body(n_seq, n_ten, *args):
    hidden, w_query, post_gain, cache_pool, prompt_cache = args[0], args[2], args[6], args[7], args[8]
    fits = (
        n_seq == 4
        and n_ten == 4
        and w_query.shape[1] == SUB * HD
        and post_gain.shape[0] % LANES == 0
        and cache_pool.shape[2] == LANES
        and cache_pool.shape[0] % SUB == 0
        and LANES % prompt_cache.shape[2] == 0
        and prompt_cache.shape[2] % (2 * SUB) == 0
        and args[9].shape[0] == LANES == hidden.shape[0] * n_seq
        and args[11].shape[1] % SUB == 0
        and prompt_cache.shape[0] <= CODE
        and cache_pool.shape[0] <= LANES
        and hidden.shape[0] % (2 * SUB) == 0
    )
    if fits:
        return fast_body(n_seq, n_ten, *args)
    return plain_body(*args)


def solution(mesh):
    return jax.shard_map(
        functools.partial(body, mesh.shape["seq"], mesh.shape["tensor"]),
        mesh=mesh,
        in_specs=(
            P(("groups", "seq"), None),
            P(),
            P(None, "tensor"),
            P(None, "tensor"),
            P(None, "tensor"),
            P("tensor", None),
            P("tensor"),
            P(("groups", "seq"), None, None, "tensor"),
            P("seq", None, None, "tensor"),
            P("groups"),
            P("groups"),
            P("groups", None),
        ),
        out_specs=(P(("groups", "seq"), "tensor"), P(("groups", "seq"), None, "tensor")),
        check_vma=False,
    )
```
